32 devices in a mesh: dp: 8 (over z, x), cand: 4 (over y, core).
Axes of the slice: x: 2, y: 2, z: 4, core: 2. Of those that a mesh axis runs over, the one named last changes fastest.
Arguments:
- hidden: bfloat16 [16, 32, 128, 768], P('dp', 'cand'), may hold values from -24 to 24
- attn_weight: bfloat16 [768, 3072], P('dp'), may hold values from -1 to 1
- norm_gain: float32 [768], replicated, may hold values from 0.2 to 4
- pos_bias: float32 [12, 128, 128], replicated, may hold values from -5 to 5
- score_weight: float32 [768], replicated, may hold values from -4 to 4
- pair_lengths: int32 [16, 32], P('dp', 'cand'), may hold values from 32 to 128
- labels: int32 [16, 32], P('dp', 'cand'), may hold values from 0 to 3
Outputs:
- update: float32 [768, 3072], P('dp')
- loss: float32 [16], P('dp')
The draws below stay inside these ranges and needn't reach their ends.
All inputs are finite; a program needn't handle non-finite values.
Results may differ from the reference program's by a relative error of at most 0.017.
Values may be sent and summed in bfloat16 or wider, within the bound.
A program may use at most 128 MiB of HBM per device.

```python
import jax
import jax.numpy as jnp
from jax import lax

D = 768
HEADS = 12
HEAD = 64
SEQ = 128
CANDS = 32
QUERIES = 16


def draw_norm_gain(key, part):
    place = jnp.arange(D, dtype=jnp.int32).astype(jnp.float32) / jnp.float32(D)
    jitter = jax.random.uniform(jax.random.fold_in(key, 7401), (D,), jnp.float32, 0.75, 1.25)
    lowest, highest = (0.4, 2.0)
    values = jnp.exp(jnp.log(lowest) + (jnp.log(highest) - jnp.log(lowest)) * place) * jitter
    return jnp.clip(values, 0.2, 4.0)


def draw_score_weight(key, part):
    values = jax.random.normal(jax.random.fold_in(key, 7102), (D,), jnp.float32)
    values = jnp.clip(values, -6.0, 6.0) * jnp.sqrt(4.0 / jnp.float32(D))
    return jnp.clip(values, -4.0, 4.0)


def draw_attn_weight(key, part):
    values = jax.random.normal(jax.random.fold_in(key, 7301), (D, 4 * D), jnp.float32)
    values = jnp.clip(values, -6.0, 6.0) / jnp.sqrt(jnp.float32(D))
    column = jnp.arange(4 * D, dtype=jnp.int32)
    factor = jnp.where(column < D, 1.0 / jnp.sqrt(jnp.float32(HEAD)), 1.0)
    values = jnp.clip(values * factor[None, :], -1.0, 1.0)
    return values.astype(jnp.bfloat16)


def draw_hidden(key, part):
    normal_part = jax.random.normal(jax.random.fold_in(key, 7201), (QUERIES, CANDS, SEQ, D), jnp.float32)
    normal_part = jnp.clip(normal_part, -6.0, 6.0)
    values = normal_part
    return jnp.clip(values, -24.0, 24.0).astype(jnp.bfloat16)


def touch_ends(drawn, rng, least, largest):
    extent = drawn.shape
    index_at = [jax.random.randint(jax.random.fold_in(rng, axis), (), 0, extent[axis]) for axis in range(len(extent))]
    drawn = drawn.at[tuple(index_at)].set(least)
    longest = extent.index(max(extent))
    index_at[longest] = (index_at[longest] + 1) % extent[longest]
    return drawn.at[tuple(index_at)].set(largest)


def gaussian(stream_key, dims, scale, bound, kind=jnp.bfloat16):
    entries = jax.random.normal(stream_key, dims, jnp.float32) * scale
    return jnp.minimum(jnp.maximum(entries, -bound), bound).astype(kind)


def setup_inputs(seed: int = 0) -> dict:
    key_list = jax.random.split(jax.random.key(seed), 8)
    return {
        "hidden": draw_hidden(jax.random.fold_in(key_list[7], 71), 0),
        "attn_weight": draw_attn_weight(jax.random.fold_in(key_list[7], 71), 0),
        "norm_gain": draw_norm_gain(jax.random.fold_in(key_list[7], 71), 0),
        "pos_bias": gaussian(key_list[3], (HEADS, SEQ, SEQ), 1.0, 5.0, jnp.float32),
        "score_weight": draw_score_weight(jax.random.fold_in(key_list[7], 71), 0),
        "pair_lengths": touch_ends(jax.random.randint(key_list[5], (QUERIES, CANDS), SEQ // 4, SEQ + 1), jax.random.fold_in(key_list[5], 1), SEQ // 4, SEQ).astype(jnp.int32),
        "labels": touch_ends(jax.random.randint(key_list[6], (QUERIES, CANDS), 0, 4), jax.random.fold_in(key_list[6], 1), 0, 3).astype(jnp.int32),
    }


EPS = 1e-06

def rms_rows(values, gain):
    factor = lax.rsqrt(lax.optimization_barrier(jnp.mean(values * values, axis=-1, keepdims=True)) + EPS)
    return values * factor * gain

def attend(qkv, pos_bias, pair_len):
    batch, seq, triple = qkv.shape
    width = triple // 3
    heads = pos_bias.shape[0]
    head_size = width // heads
    parts = qkv.reshape(batch, seq, 3, heads, head_size).astype(jnp.float32)
    logits = jnp.einsum('bqhd,bkhd->bhqk', parts[:, :, 0], parts[:, :, 1])
    logits = logits + pos_bias[None]
    valid = jnp.arange(seq, dtype=jnp.int32)[None, :] < pair_len[:, None]
    logits = jnp.where(valid[:, None, None, :], logits, -1e+30)
    highest = lax.optimization_barrier(jnp.max(logits, axis=-1, keepdims=True))
    expo = jnp.exp(logits - highest)
    probs = (expo / lax.optimization_barrier(jnp.sum(expo, axis=-1, keepdims=True))).astype(jnp.bfloat16)
    context = jnp.einsum('bhqk,bkhd->bqhd', probs.astype(jnp.float32), parts[:, :, 2])
    return context.astype(jnp.bfloat16).reshape(batch, seq, width)

def forward(tokens, weights, norm_gain, pos_bias, pair_len):
    batch, seq, width = tokens.shape
    values = tokens.astype(jnp.float32)
    normed = rms_rows(values, norm_gain).astype(jnp.bfloat16)
    qkv = jnp.dot(normed.reshape(-1, width), weights[:, :3 * width], preferred_element_type=jnp.float32)
    qkv = qkv.astype(jnp.bfloat16).reshape(batch, seq, 3 * width)
    context = attend(qkv, pos_bias, pair_len)
    out_rows = values + jnp.dot(context.reshape(-1, width), weights[:, 3 * width:], preferred_element_type=jnp.float32).reshape(batch, seq, width)
    live = (jnp.arange(seq, dtype=jnp.int32)[None, :] < pair_len[:, None]).astype(jnp.float32)
    share = live / pair_len.astype(jnp.float32)[:, None]
    pooled = lax.optimization_barrier(jnp.sum(out_rows * share[:, :, None], axis=1))
    return (normed, qkv, context, pooled, share)

def score_head(pooled, score_weight):
    return lax.optimization_barrier(jnp.sum(rms_rows(pooled, 1.0) * score_weight, axis=-1))

def backward(normed, qkv, context, pooled, share, weights, pos_bias, pair_len, score_weight, score_grad):
    batch, seq, width = normed.shape
    unused, head_back = jax.vjp(lambda vector: score_head(vector, score_weight), pooled)
    pooled_grad = head_back(score_grad)[0]
    out_grad = (pooled_grad[:, None, :] * share[:, :, None]).astype(jnp.bfloat16)
    flat_out = out_grad.reshape(-1, width)
    context_grad = jnp.dot(flat_out, weights[:, 3 * width:].T, preferred_element_type=jnp.float32)
    context_grad = context_grad.astype(jnp.bfloat16).reshape(batch, seq, width)
    unused2, attend_back = jax.vjp(lambda block: attend(block, pos_bias, pair_len), qkv)
    qkv_grad = attend_back(context_grad)[0].reshape(-1, 3 * width)
    first = jnp.dot(normed.reshape(-1, width).T, qkv_grad, preferred_element_type=jnp.float32)
    second = jnp.dot(context.reshape(-1, width).T, flat_out, preferred_element_type=jnp.float32)
    return jnp.concatenate([first, second], axis=1)

def reference(hidden, attn_weight, norm_gain, pos_bias, score_weight, pair_lengths, labels):
    width = hidden.shape[3]

    def scores_of(pair):
        tokens, pair_len = pair
        unused_a, unused_b, unused_c, pooled, unused_d = forward(tokens, attn_weight, norm_gain, pos_bias, pair_len)
        return score_head(pooled, score_weight)
    scores = lax.map(scores_of, (hidden, pair_lengths))
    highest = lax.optimization_barrier(jnp.max(scores, axis=1, keepdims=True))
    expsum = lax.optimization_barrier(jnp.sum(jnp.exp(scores - highest), axis=1, keepdims=True))
    target = jnp.exp(labels.astype(jnp.float32))
    target_sum = lax.optimization_barrier(jnp.sum(target, axis=1, keepdims=True))
    target_dot = lax.optimization_barrier(jnp.sum(target * scores, axis=1, keepdims=True))
    loss = (highest + jnp.log(expsum) - target_dot / target_sum)[:, 0]
    score_grad = jnp.exp(scores - highest) / expsum - target / target_sum

    def accumulate(total, pair):
        tokens, pair_len, grad_row = pair
        normed, qkv, context, pooled, share = forward(tokens, attn_weight, norm_gain, pos_bias, pair_len)
        term = backward(normed, qkv, context, pooled, share, attn_weight, pos_bias, pair_len, score_weight, grad_row)
        return (total + term, None)
    start = jnp.zeros((width, 4 * width), jnp.float32)
    grad, unused = lax.scan(accumulate, start, (hidden, pair_lengths, score_grad))
    rms_value = jnp.sqrt(jnp.sum(grad * grad) / (4.0 * width * width))
    update = grad / (rms_value + EPS)
    return (update, loss)
```

```python
import functools

import jax
import jax.numpy as jnp
from jax import lax
from jax.experimental import pallas as pl
from jax.experimental.pallas import tpu as pltpu
from jax.sharding import PartitionSpec as P

EPS = 1e-06
F32 = jnp.float32
BF16 = jnp.bfloat16
VMEM_LIMIT = 60 * 1024 * 1024
NT = (((1,), (1,)), ((), ()))
TN = (((0,), (0,)), ((), ()))
MESH = pl.DeviceIdType.MESH


def half_masks(lanes):
    lane = lax.broadcasted_iota(jnp.int32, (1, lanes), 1)
    low = (lane < lanes // 2).astype(F32)
    return low.astype(BF16), (1.0 - low).astype(BF16)


def stack_halves(block, low, high):
    return jnp.concatenate([block * low, block * high], axis=0)


def head_mask(hpad, width, head_size):
    lane = lax.broadcasted_iota(jnp.int32, (hpad, width), 1)
    head = lax.broadcasted_iota(jnp.int32, (hpad, width), 0)
    start = head * head_size
    return ((lane >= start) & (lane < start + head_size)).astype(F32)


def arrived(ref, sem):
    pltpu.make_async_copy(ref, ref, sem).wait()


def push(src, dst, send, recv, target):
    pltpu.make_async_remote_copy(
        src_ref=src, dst_ref=dst, send_sem=send, recv_sem=recv, device_id=target, device_id_type=MESH
    ).start()


def lengths_column(ref, pairs, per):
    row = lax.broadcasted_iota(jnp.int32, (pairs, 1), 0)
    column = jnp.zeros((pairs, 1), F32)
    for i in range(pairs):
        column = jnp.where(row == i, ref[i // per, i % per].astype(F32), column)
    return column


def fused_kernel(n, m, early, len_ref, lab_ref, h_hbm, w_hbm, gain_ref, bias_hbm, sw_ref,
                 fin, scale_ref, loss_ref,
                 h_scr, bias_scr, w_scr, norm_scr, nt_scr, qk_scr, p_scr, wsum_scr, u_scr, hsum_scr, ex_scr,
                 dp_scr, dqk_scr, grads, r1, s1, r2, s2, r3, s3, r4, sq, r6,
                 h_sem, b_sem, wa_sem, wb_sem,
                 za_s, za_r, xa_s, xa_r, ca_s, zb_s, zb_r, xb_s, xb_r, yb_s, cb_s, g_r, ex_s, ex_r,
                 t1, v1, t2, v2, t3, v3, t4, v4, t5, v5, t6, v6):
    pairs, seq, width = h_scr.shape
    queries, per = len_ref.shape
    heads = bias_scr.shape[0]
    groups, half, _, rows, lanes = w_scr.shape
    duos = heads // 2
    duo = m // 2
    head_size = width // heads
    hpad = u_scr.shape[1]
    batch = pairs // h_sem.shape[0]
    batches = pairs // batch
    early_rounds = early // 2
    late_rounds = (groups - early) // m
    d, c = lax.axis_index("dp"), lax.axis_index("cand")
    z, x = d // 2, d % 2
    y, core = c // 2, c % 2
    across = (d + 1 - 2 * x, c)
    other = (d, c + 1 - 2 * core)

    def column(g):
        late = g // (2 * duos)
        return (1 - late) * (g // 2 + (g % 2) * duos) + late * g

    def early_group(a):
        return 2 * a + core

    def late_group(r):
        return early + r * m + c

    def load(g, sem):
        at = pl.multiple_of(column(g) * lanes, lanes)
        return pltpu.make_async_copy(w_hbm.at[:, pl.ds(at, lanes)], w_scr.at[g, z, x], sem)

    loads = [load(early_group(a), wa_sem.at[a]) for a in range(early_rounds)]
    loads += [load(late_group(r), wb_sem.at[r]) for r in range(late_rounds)]
    tokens = []
    for b in range(batches):
        part = pl.ds(b * batch, batch)
        tokens.append(pltpu.make_async_copy(h_hbm.at[part], h_scr.at[part], h_sem.at[b]))
    bias_load = pltpu.make_async_copy(bias_hbm, bias_scr, b_sem)
    for copy in loads[:1] + tokens[:1] + loads[1:] + tokens[1:] + [bias_load]:
        copy.start()
    peers = [(d, lax.rem(c + j, m)) for j in range(1, m)] + [(lax.rem(d + j, n), c) for j in range(1, n)]
    barrier = pltpu.get_barrier_semaphore()
    for peer in peers:
        pl.semaphore_signal(barrier, inc=1, device_id=peer, device_id_type=MESH)

    col = lax.broadcasted_iota(jnp.int32, (1, seq), 1)
    row = lax.broadcasted_iota(jnp.int32, (seq, 1), 0)
    low, high = half_masks(lanes)
    gain = gain_ref[...].reshape(1, width)
    sw = sw_ref[...].reshape(1, width)

    def length_of(i):
        return len_ref[i // per, i % per]

    def normalise(b):
        tokens[b].wait()
        values = h_scr[b * batch : (b + 1) * batch].reshape(batch * seq, width).astype(F32)
        factor = lax.rsqrt(jnp.mean(values * values, axis=-1, keepdims=True) + EPS)
        normed = (values * factor * gain).astype(BF16)
        norm_scr[b * batch : (b + 1) * batch] = normed.reshape(batch, seq, width)
        nt_scr[:, b * batch * seq : (b + 1) * batch * seq] = normed.T
        for j in range(batch):
            i = b * batch + j
            live = (row < length_of(i)).astype(F32)
            hsum_scr[i : i + 1, :] = jnp.sum(values[j * seq : (j + 1) * seq] * live, axis=0, keepdims=True)

    def send_z(g, s, r):
        for j in range(1, half):
            block = w_scr.at[g, z, x]
            push(block, block, s, r, (2 * lax.rem(z + j, half) + x, c))

    def relay_x(g, z_sem, s, r):
        arrived(w_scr.at[g, 0 : half - 1, 0], z_sem)
        blocks = w_scr.at[g, :, x]
        push(blocks, blocks, s, r, across)

    def early_x(a):
        relay_x(early_group(a), za_r.at[a], xa_s.at[a], xa_r.at[a])

    def early_core(a):
        g = early_group(a)
        arrived(w_scr.at[g, :, 0], xa_r.at[a])
        push(w_scr.at[g], w_scr.at[g], ca_s.at[a], g_r.at[g], other)

    def early_ready(a):
        g = 2 * a + 1 - core
        arrived(w_scr.at[g], g_r.at[g])

    def late_x(r):
        relay_x(late_group(r), zb_r.at[r], xb_s.at[r], xb_r.at[r])

    def late_y(r):
        g = late_group(r)
        arrived(w_scr.at[g, :, 0], xb_r.at[r])
        for j in range(1, duo):
            push(w_scr.at[g], w_scr.at[g], yb_s.at[r, j - 1], g_r.at[g], (d, 2 * lax.rem(y + j, duo) + core))
        push(w_scr.at[g], w_scr.at[g], cb_s.at[r, 0], g_r.at[g], other)

    def late_core(r):
        for j in range(1, duo):
            g = early + r * m + 2 * lax.rem(y - j + duo, duo) + core
            arrived(w_scr.at[g], g_r.at[g])
            push(w_scr.at[g], w_scr.at[g], cb_s.at[r, j], g_r.at[g], other)

    def late_ready(r):
        for j in range(duo):
            g = early + r * m + 2 * j + 1 - core
            arrived(w_scr.at[g], g_r.at[g])

    normalise(0)
    pl.semaphore_wait(barrier, len(peers))
    for a in range(early_rounds):
        loads[a].wait()
        send_z(early_group(a), za_s.at[a], za_r.at[a])
    for r in range(late_rounds):
        loads[early_rounds + r].wait()
        send_z(late_group(r), zb_s.at[r], zb_r.at[r])
    for b in range(1, batches):
        normalise(b)
    early_x(0)
    if early_rounds > 1:
        early_x(1)
    bias_load.wait()
    early_core(0)

    def weight(g):
        value = w_scr[g]
        if rows % 16 == 0:
            return value.reshape(width, lanes)
        return value.astype(F32).reshape(width, lanes).astype(BF16)

    def project(hp, b):
        block = norm_scr[b * batch : (b + 1) * batch].reshape(batch * seq, width)
        both = jnp.concatenate([weight(2 * hp), weight(2 * hp + 1)], axis=1)
        proj = jnp.dot(block, both, preferred_element_type=F32)
        qk_scr[hp, b * batch : (b + 1) * batch] = proj.astype(BF16).reshape(batch, seq, 2 * lanes)

    def attend(hp, i):
        length = length_of(i)
        penalty = jnp.where(col < length, 0.0, 1.0) > 0.5
        live = (row < length).astype(F32)
        live2 = jnp.concatenate([live] * 2, axis=0)
        q2 = qk_scr[hp, i, :, :lanes]
        k2 = qk_scr[hp, i, :, lanes:]
        logits = lax.dot_general(stack_halves(q2, low, high), k2, NT, preferred_element_type=F32)
        logits = logits + bias_scr[pl.ds(2 * hp, 2)].reshape(2 * seq, seq)
        logits = jnp.where(penalty, -1e30, logits)
        expo = jnp.exp(logits - jnp.max(logits, axis=-1, keepdims=True))
        inv = live2 / jnp.sum(expo, axis=-1, keepdims=True)
        probs = (expo * inv).astype(BF16)
        p_scr[hp, i] = probs.reshape(2, seq, seq)
        wsum_scr[hp, i] = jnp.sum(probs.astype(F32).reshape(2, seq, seq), axis=1)

    def forward_step(hp, carry):
        @pl.when(hp + 2 < early_rounds)
        def _():
            early_x(hp + 2)

        @pl.when(hp < early_rounds)
        def _():
            early_ready(hp)

        @pl.when(hp == early_rounds)
        def _():
            late_ready(0)

        for b in range(batches):
            if b == batches // 2:
                @pl.when((hp >= 1) & (hp - 1 < late_rounds))
                def _():
                    late_x(hp - 1)

                @pl.when((hp >= 3) & (hp - 3 < late_rounds))
                def _():
                    late_core(hp - 3)

            if b == batches // 4:
                @pl.when(hp + 1 < early_rounds)
                def _():
                    early_core(hp + 1)

                @pl.when((hp >= 2) & (hp - 2 < late_rounds))
                def _():
                    late_y(hp - 2)

            project(hp, b)
            for j in range(batch):
                attend(hp, b * batch + j)
        return carry

    lax.fori_loop(0, duos, forward_step, 0)
    for r in range(max(duos - 3, 0), late_rounds):
        late_core(r)
    for i in range(pairs):
        parts = [wsum_scr[j, i] for j in range(duos)]
        if hpad > heads:
            parts.append(jnp.zeros((hpad - heads, seq), F32))
        weights = jnp.concatenate(parts, axis=0).astype(BF16)
        u_scr[i] = jnp.dot(weights, norm_scr[i], preferred_element_type=F32).astype(BF16)
    for r in range(1, late_rounds):
        late_ready(r)

    w_v = jnp.concatenate([weight(2 * duos + j) for j in range(duos)], axis=1)
    w_o = jnp.concatenate([weight(3 * duos + j) for j in range(duos)], axis=1)
    u = u_scr[...].reshape(pairs * hpad, width)
    mixed = jnp.dot(u, w_v, preferred_element_type=F32)
    mask = head_mask(hpad, width, head_size)
    ctx32 = jnp.sum(mixed.reshape(pairs, hpad, width) * mask[None], axis=1)
    ctx = ctx32.astype(BF16)
    share = 1.0 / lengths_column(len_ref, pairs, per)
    mean = ctx32 * share
    mean_high = mean.astype(BF16)
    mean_low = (mean - mean_high.astype(F32)).astype(BF16)
    both = jnp.dot(jnp.concatenate([mean_high, mean_low], axis=0), w_o, preferred_element_type=F32)
    pooled = hsum_scr[...] * share + both[:pairs] + both[pairs:]
    factor = lax.rsqrt(jnp.mean(pooled * pooled, axis=-1, keepdims=True) + EPS)
    score = jnp.sum(pooled * factor * sw, axis=-1, keepdims=True)
    label = lengths_column(lab_ref, pairs, per)
    score = jnp.broadcast_to(score, (pairs, lanes))
    label = jnp.broadcast_to(label, (pairs, lanes))
    ex_scr[c] = jnp.concatenate([score, label], axis=0)
    for j in range(1, m):
        push(ex_scr.at[c], ex_scr.at[c], ex_s.at[j - 1], ex_r.at[j - 1], (d, lax.rem(c + j, m)))

    dot = jnp.sum(pooled * sw, axis=-1, keepdims=True) * (1.0 / width)
    slope = (factor * sw - pooled * (factor * factor * factor * dot)) * share
    cg = lax.dot_general(slope.astype(BF16), w_o, NT, preferred_element_type=F32)
    spread = (cg[:, None, :] * mask[None]).astype(BF16).reshape(pairs * hpad, width)
    wc = lax.dot_general(spread, w_v, NT, preferred_element_type=F32)
    u_scr_wc = wc.astype(BF16).reshape(pairs, hpad, width)
    for i in range(pairs):
        part = jnp.dot(u_scr_wc[i], nt_scr[:, i * seq : (i + 1) * seq], preferred_element_type=F32)
        for j in range(duos):
            dp_scr[j, i] = part[2 * j : 2 * j + 2]

    for j in range(1, m):
        arrived(ex_scr.at[lax.rem(c - j + m, m)], ex_r.at[j - 1])
    all_scores, all_labels = ex_scr[:, :pairs], ex_scr[:, pairs:]
    target = jnp.exp(all_labels)
    own_target = jnp.exp(label)
    query = lax.broadcasted_iota(jnp.int32, (pairs, lanes), 0) // per
    loss_row = lax.broadcasted_iota(jnp.int32, loss_ref.shape, 0)
    loss = jnp.zeros(loss_ref.shape, F32)
    score_grad = jnp.zeros((pairs, lanes), F32)

    def total(values):
        return jnp.sum(jnp.sum(values, axis=0), axis=0, keepdims=True)

    for q in range(queries):
        inside = (query == q)[None]
        highest = jnp.max(jnp.max(jnp.where(inside, all_scores, -3e38), axis=0), axis=0, keepdims=True)
        expsum = total(jnp.where(inside, jnp.exp(all_scores - highest[None]), 0.0))
        target_sum = total(jnp.where(inside, target, 0.0))
        target_dot = total(jnp.where(inside, target * all_scores, 0.0))
        loss = jnp.where(loss_row == q, highest + jnp.log(expsum) - target_dot / target_sum, loss)
        own = jnp.exp(score - highest) / expsum - own_target / target_sum
        score_grad = jnp.where(query == q, own, score_grad)
    loss_ref[...] = loss
    sg = score_grad[:, :1]
    out_grad = (slope * sg).astype(BF16)
    spread = (cg * sg).astype(BF16).astype(F32)
    spread = (spread[:, None, :] * mask[None]).astype(BF16).reshape(pairs * hpad, width)
    gv = lax.dot_general(u, spread, TN, preferred_element_type=F32).astype(BF16)
    go = lax.dot_general(ctx, out_grad, TN, preferred_element_type=F32).astype(BF16)
    for t in range(2 * duos):
        source = (gv, go)[t // duos]
        at = (t % duos) * lanes
        grads[t // 2, t % 2] = source[:, at : at + lanes].reshape(half, 2, rows, lanes)
    for i in range(pairs):
        for j in range(duos):
            dp_scr[j, i] = dp_scr[j, i] * sg[i : i + 1]

    chunks = r1.shape[0]

    def stage_core(k):
        push(grads.at[k * duo : (k + 1) * duo, 1 - core], r1.at[k], t1.at[k], v1.at[k], other)

    def stage_y(k):
        arrived(r1.at[k], v1.at[k])
        s1[k] = (grads[k * duo : (k + 1) * duo, core].astype(F32) + r1[k].astype(F32)).astype(BF16)
        for j in range(1, duo):
            peer = lax.rem(y + j, duo)
            push(s1.at[k, peer], r2.at[k, j - 1], t2.at[k, j - 1], v2.at[k, j - 1], (d, 2 * peer + core))

    def stage_x(k):
        value = s1[k, y].astype(F32)
        for j in range(1, duo):
            arrived(r2.at[k, j - 1], v2.at[k, j - 1])
            value = value + r2[k, j - 1].astype(F32)
        s2[k] = value.astype(BF16)
        push(s2.at[k, :, 1 - x], r3.at[k], t3.at[k], v3.at[k], across)

    def stage_z(k):
        arrived(r3.at[k], v3.at[k])
        s3[k] = (s2[k, :, x].astype(F32) + r3[k].astype(F32)).astype(BF16)
        for j in range(1, half):
            peer = lax.rem(z + j, half)
            push(s3.at[k, peer], r4.at[k, j - 1], t4.at[k, j - 1], v4.at[k, j - 1], (2 * peer + x, c))

    def stage_cand(k):
        value = s3[k, z].astype(F32)
        for j in range(1, half):
            arrived(r4.at[k, j - 1], v4.at[k, j - 1])
            value = value + r4[k, j - 1].astype(F32)
        fin[k * m + c] = value.astype(BF16)
        for j in range(1, m):
            piece = fin.at[k * m + c]
            push(piece, piece, t5.at[k, j - 1], v5.at[k, j - 1], (d, lax.rem(c + j, m)))

    stages = (stage_core, stage_y, stage_x, stage_z, stage_cand)
    places = batches + 1
    plan = stage_slots(duos, chunks, m, places)
    last = places * duos

    def run(hp, place):
        for step in range(duos):
            items = [item for item in plan if item[0] == places * step + place]
            if items:
                @pl.when(hp == step)
                def _():
                    for _, stage, k in items:
                        stages[stage](k)

    def backward_step(hp, carry):
        for b in range(batches):
            run(hp, b)
            for j in range(batch):
                i = b * batch + j
                probs = p_scr[hp, i].astype(F32)
                term = probs * dp_scr[hp, i][:, None, :]
                dlog = (term - probs * jnp.sum(term, axis=-1, keepdims=True)).astype(BF16)
                wide = jnp.concatenate([dlog[0], dlog[1]], axis=1)
                q2 = stack_halves(qk_scr[hp, i, :, :lanes], low, high)
                k2 = stack_halves(qk_scr[hp, i, :, lanes:], low, high)
                dq = jnp.dot(wide, k2, preferred_element_type=F32)
                dk = lax.dot_general(dlog.reshape(2 * seq, seq), q2, TN, preferred_element_type=F32)
                dqk_scr[i, :, :lanes] = dq.astype(BF16)
                dqk_scr[i, :, lanes:] = dk.astype(BF16)
        grad = jnp.dot(nt_scr[...], dqk_scr[...].reshape(pairs * seq, 2 * lanes), preferred_element_type=F32)
        grads[duos + hp, 0] = grad[:, :lanes].reshape(half, 2, rows, lanes).astype(BF16)
        grads[duos + hp, 1] = grad[:, lanes:].reshape(half, 2, rows, lanes).astype(BF16)
        run(hp, batches)
        return carry

    lax.fori_loop(0, duos, backward_step, 0)
    for slot, stage, k in plan:
        if slot >= last:
            stages[stage](k)
    for k in range(chunks):
        for j in range(1, m):
            arrived(fin.at[k * m + lax.rem(c - j + m, m)], v5.at[k, j - 1])
    part = jnp.zeros((8, lanes), F32)
    for g in range(groups):
        block = fin[g].astype(F32).reshape(rows // 8, 8, lanes)
        part = part + jnp.sum(block * block, axis=0)
    sq[...] = part
    r6[d] = part
    for j in range(1, n):
        push(sq, r6.at[d], t6.at[j - 1], v6.at[j - 1], (lax.rem(d + j, n), c))
    for j in range(1, n):
        arrived(r6.at[lax.rem(d - j + n, n)], v6.at[j - 1])
    count = groups * lanes * n * rows
    squares = jnp.sum(jnp.sum(jnp.sum(r6[...], axis=0), axis=0, keepdims=True), axis=1, keepdims=True)
    scale_ref[...] = jnp.broadcast_to(1.0 / (jnp.sqrt(squares / count) + EPS), scale_ref.shape)

    for a in range(early_rounds):
        arrived(w_scr.at[0, 0 : half - 1, 0], za_s.at[a])
        arrived(w_scr.at[0, :, 0], xa_s.at[a])
        arrived(w_scr.at[0], ca_s.at[a])
    for r in range(late_rounds):
        arrived(w_scr.at[0, 0 : half - 1, 0], zb_s.at[r])
        arrived(w_scr.at[0, :, 0], xb_s.at[r])
        for j in range(duo - 1):
            arrived(w_scr.at[0], yb_s.at[r, j])
        for j in range(duo):
            arrived(w_scr.at[0], cb_s.at[r, j])
    for j in range(m - 1):
        arrived(ex_scr.at[c], ex_s.at[j])
    for k in range(chunks):
        arrived(r1.at[k], t1.at[k])
        arrived(r3.at[k], t3.at[k])
        for j in range(duo - 1):
            arrived(r2.at[k, j], t2.at[k, j])
        for j in range(half - 1):
            arrived(r4.at[k, j], t4.at[k, j])
        for j in range(m - 1):
            arrived(fin.at[k * m + c], t5.at[k, j])
    for j in range(n - 1):
        arrived(sq, t6.at[j])


def stage_slots(duos, chunks, m, places):
    plan = []
    previous = [0] * 5
    for k in range(chunks):
        done = (k + 1) * m - 2 * duos
        first = 0 if done <= 0 else places * (-(-done // 2)) - 1
        slots = [first]
        for gap in (2, 6, 4, 4):
            slots.append(slots[-1] + gap)
        for stage in range(5):
            slots[stage] = max(slots[stage], previous[stage] + (0 if stage == 0 else 3))
            if stage:
                slots[stage] = max(slots[stage], slots[stage - 1] + 1)
            plan.append((slots[stage], stage, k))
        previous = slots
    return sorted(plan)


def finish_kernel(duos, fin, scale_ref, loss_in, out_ref, loss_ref):
    groups, rows, lanes = fin.shape
    scale = scale_ref[0:1, :]
    for at in range(groups):
        if at < 2 * duos:
            col = 2 * duos + at
        else:
            col = (at % 2) * duos + (at - 2 * duos) // 2
        out_ref[:, col * lanes : (col + 1) * lanes] = fin[at].astype(F32) * scale
    for q in range(loss_ref.shape[0]):
        loss_ref[q] = jnp.max(loss_in[q : q + 1, :])


def shards(hidden, attn_weight, norm_gain, pos_bias, score_weight, pair_lengths, labels):
    queries, per, seq, width = hidden.shape
    pairs = queries * per
    heads = pos_bias.shape[0]
    n, m = lax.axis_size("dp"), lax.axis_size("cand")
    lanes = 2 * (width // heads)
    duos = heads // 2
    groups = 4 * duos
    rows, half, duo = width // n, n // 2, m // 2
    early = groups // 3
    early_rounds, late_rounds = early // 2, (groups - early) // m
    batch = 4 if pairs % 4 == 0 else 1
    hpad = -(-heads // 16) * 16
    chunks = groups // m
    near, far = max(duo - 1, 1), max(half - 1, 1)
    dma = pltpu.SemaphoreType.DMA
    vmem = pltpu.VMEM
    here = pl.BlockSpec(memory_space=pltpu.VMEM)
    away = pl.BlockSpec(memory_space=pl.ANY)
    small = pl.BlockSpec(memory_space=pltpu.SMEM)
    loss_rows = -(-queries // 8) * 8
    fin, scale, loss = pl.pallas_call(
        functools.partial(fused_kernel, n, m, early),
        in_specs=[small, small, away, away, here, away, here],
        out_specs=[here, here, here],
        out_shape=[
            jax.ShapeDtypeStruct((groups, rows, lanes), BF16),
            jax.ShapeDtypeStruct((8, lanes), F32),
            jax.ShapeDtypeStruct((loss_rows, lanes), F32),
        ],
        scratch_shapes=[
            vmem((pairs, seq, width), BF16),
            vmem(pos_bias.shape, F32),
            vmem((groups, half, 2, rows, lanes), BF16),
            vmem((pairs, seq, width), BF16),
            vmem((width, pairs * seq), BF16),
            vmem((duos, pairs, seq, 2 * lanes), BF16),
            vmem((duos, pairs, 2, seq, seq), BF16),
            vmem((duos, pairs, 2, seq), F32),
            vmem((pairs, hpad, width), BF16),
            vmem((pairs, width), F32),
            vmem((m, 2 * pairs, lanes), F32),
            vmem((duos, pairs, 2, seq), F32),
            vmem((pairs, seq, 2 * lanes), BF16),
            vmem((2 * duos, 2, half, 2, rows, lanes), BF16),
            vmem((chunks, duo, half, 2, rows, lanes), BF16),
            vmem((chunks, duo, half, 2, rows, lanes), BF16),
            vmem((chunks, near, half, 2, rows, lanes), BF16),
            vmem((chunks, half, 2, rows, lanes), BF16),
            vmem((chunks, half, rows, lanes), BF16),
            vmem((chunks, half, rows, lanes), BF16),
            vmem((chunks, far, rows, lanes), BF16),
            vmem((8, lanes), F32),
            vmem((n, 8, lanes), F32),
            dma((pairs // batch,)), dma, dma((early_rounds,)), dma((late_rounds,)),
            dma((early_rounds,)), dma((early_rounds,)), dma((early_rounds,)), dma((early_rounds,)),
            dma((early_rounds,)),
            dma((late_rounds,)), dma((late_rounds,)), dma((late_rounds,)), dma((late_rounds,)),
            dma((late_rounds, near)), dma((late_rounds, duo)), dma((groups,)),
            dma((m - 1,)), dma((m - 1,)),
            dma((chunks,)), dma((chunks,)),
            dma((chunks, near)), dma((chunks, near)),
            dma((chunks,)), dma((chunks,)),
            dma((chunks, far)), dma((chunks, far)),
            dma((chunks, m - 1)), dma((chunks, m - 1)),
            dma((n - 1,)), dma((n - 1,)),
        ],
        compiler_params=pltpu.CompilerParams(
            collective_id=0, has_side_effects=True, vmem_limit_bytes=VMEM_LIMIT
        ),
        name="fused_step",
    )(pair_lengths, labels, hidden.reshape(pairs, seq, width), attn_weight, norm_gain, pos_bias, score_weight)
    update, loss = pl.pallas_call(
        functools.partial(finish_kernel, duos),
        in_specs=[here, here, here],
        out_specs=[here, small],
        out_shape=[
            jax.ShapeDtypeStruct((rows, 4 * width), F32),
            jax.ShapeDtypeStruct((queries,), F32),
        ],
        name="finish",
    )(fin, scale, loss)
    return (update, loss)


def solution(mesh):
    in_specs = (
        P("dp", "cand", None, None),
        P("dp", None),
        P(),
        P(),
        P(),
        P("dp", "cand"),
        P("dp", "cand"),
    )
    out_specs = (P("dp", None), P("dp"))
    return jax.shard_map(shards, mesh=mesh, in_specs=in_specs, out_specs=out_specs, check_vma=False)
```

```python
import functools

import jax
import jax.numpy as jnp
from jax import lax
from jax.experimental import pallas as pl
from jax.experimental.pallas import tpu as pltpu
from jax.sharding import PartitionSpec as P

EPS = 1e-06
F32 = jnp.float32
BF16 = jnp.bfloat16
VMEM_LIMIT = 60 * 1024 * 1024
NT = (((1,), (1,)), ((), ()))
TN = (((0,), (0,)), ((), ()))
MESH = pl.DeviceIdType.MESH


def half_masks(lanes):
    lane = lax.broadcasted_iota(jnp.int32, (1, lanes), 1)
    low = (lane < lanes // 2).astype(F32)
    return low.astype(BF16), (1.0 - low).astype(BF16)


def stack_halves(block, low, high):
    return jnp.concatenate([block * low, block * high], axis=0)


def head_mask(hpad, width, head_size):
    lane = lax.broadcasted_iota(jnp.int32, (hpad, width), 1)
    head = lax.broadcasted_iota(jnp.int32, (hpad, width), 0)
    start = head * head_size
    return ((lane >= start) & (lane < start + head_size)).astype(F32)


def arrived(ref, sem):
    pltpu.make_async_copy(ref, ref, sem).wait()


def push(src, dst, send, recv, target):
    pltpu.make_async_remote_copy(
        src_ref=src, dst_ref=dst, send_sem=send, recv_sem=recv, device_id=target, device_id_type=MESH
    ).start()


def lengths_column(ref, pairs, per):
    row = lax.broadcasted_iota(jnp.int32, (pairs, 1), 0)
    column = jnp.zeros((pairs, 1), F32)
    for i in range(pairs):
        column = jnp.where(row == i, ref[i // per, i % per].astype(F32), column)
    return column


def fused_kernel(n, m, early, len_ref, lab_ref, h_hbm, w_hbm, gain_ref, bias_hbm, sw_ref,
                 fin, scale_ref, loss_ref,
                 h_scr, bias_scr, w_scr, norm_scr, nt_scr, qk_scr, p_scr, wsum_scr, u_scr, hsum_scr, ex_scr,
                 dp_scr, dqk_scr, grads, r1, s1, r2, s2, r3, s3, r4, a1, b1, a2, b2, a3, a4, sq, r6,
                 h_sem, b_sem, wa_sem, wb_sem,
                 za_s, za_r, xa_s, xa_r, ca_s, zb_s, zb_r, xb_s, xb_r, yb_s, yb_r, cb_s, g_r, ex_s, ex_r,
                 t1, v1, t2, v2, t3, v3, t4, v4, t5, v5, t6, v6,
                 e1, f1, e2, f2, e3, f3, e4, f4, e5, f5):
    pairs, seq, width = h_scr.shape
    queries, per = len_ref.shape
    heads = bias_scr.shape[0]
    groups, half, _, rows, lanes = w_scr.shape
    duos = heads // 2
    duo = m // 2
    head_size = width // heads
    hpad = u_scr.shape[1]
    batch = pairs // h_sem.shape[0]
    batches = pairs // batch
    early_rounds = early // 2
    late_rounds = (groups - early) // m
    d, c = lax.axis_index("dp"), lax.axis_index("cand")
    z, x = d // 2, d % 2
    y, core = c // 2, c % 2
    across = (d + 1 - 2 * x, c)
    other = (d, c + 1 - 2 * core)

    split = early_rounds // 2
    late = duos - early_rounds

    def column(g):
        tail = g // (2 * duos)
        return (1 - tail) * (g // 2 + (g % 2) * duos) + tail * g

    def early_group(a, which):
        return 2 * (a + late * (a // split)) + which

    def late_group(r, which):
        if r == 0:
            return 2 * split + which + (early - 2 * split) * (which // (2 * late))
        return early + r * m + which

    def load(g, sem):
        at = pl.multiple_of(column(g) * lanes, lanes)
        return pltpu.make_async_copy(w_hbm.at[:, pl.ds(at, lanes)], w_scr.at[g, z, x], sem)

    loads = [load(early_group(a, core), wa_sem.at[a]) for a in range(early_rounds)]
    loads += [load(late_group(r, c), wb_sem.at[r]) for r in range(late_rounds)]
    tokens = []
    for b in range(batches):
        part = pl.ds(b * batch, batch)
        tokens.append(pltpu.make_async_copy(h_hbm.at[part], h_scr.at[part], h_sem.at[b]))
    bias_load = pltpu.make_async_copy(bias_hbm, bias_scr, b_sem)
    for copy in loads[:1] + tokens[:1] + loads[1:] + tokens[1:] + [bias_load]:
        copy.start()
    peers = [(d, lax.rem(c + j, m)) for j in range(1, m)] + [(lax.rem(d + j, n), c) for j in range(1, n)]
    barrier = pltpu.get_barrier_semaphore()
    for peer in peers:
        pl.semaphore_signal(barrier, inc=1, device_id=peer, device_id_type=MESH)

    col = lax.broadcasted_iota(jnp.int32, (1, seq), 1)
    row = lax.broadcasted_iota(jnp.int32, (seq, 1), 0)
    key = lax.broadcasted_iota(jnp.int32, (2, seq, seq), 1)
    ones = jnp.ones((16, seq), BF16)
    low, high = half_masks(lanes)
    gain = gain_ref[...].reshape(1, width)
    sw = sw_ref[...].reshape(1, width)

    def length_of(i):
        return len_ref[i // per, i % per]

    def normalise(b):
        tokens[b].wait()
        values = h_scr[b * batch : (b + 1) * batch].reshape(batch * seq, width).astype(F32)
        factor = lax.rsqrt(jnp.mean(values * values, axis=-1, keepdims=True) + EPS)
        normed = (values * factor * gain).astype(BF16)
        norm_scr[b * batch : (b + 1) * batch] = normed.reshape(batch, seq, width)
        nt_scr[:, b * batch * seq : (b + 1) * batch * seq] = normed.T
        for j in range(batch):
            i = b * batch + j
            live = (row < length_of(i)).astype(F32)
            hsum_scr[i : i + 1, :] = jnp.sum(values[j * seq : (j + 1) * seq] * live, axis=0, keepdims=True)

    def send_z(g, s, r):
        for j in range(1, half):
            block = w_scr.at[g, z, x]
            push(block, block, s, r, (2 * lax.rem(z + j, half) + x, c))

    def relay_x(g, z_sem, s, r):
        arrived(w_scr.at[g, 0 : half - 1, 0], z_sem)
        blocks = w_scr.at[g, :, x]
        push(blocks, blocks, s, r, across)

    def early_x(a):
        relay_x(early_group(a, core), za_r.at[a], xa_s.at[a], xa_r.at[a])

    def early_core(a):
        g = early_group(a, core)
        arrived(w_scr.at[g, :, 0], xa_r.at[a])
        push(w_scr.at[g], w_scr.at[g], ca_s.at[a], g_r.at[g], other)

    def early_ready(a):
        g = early_group(a, 1 - core)
        arrived(w_scr.at[g], g_r.at[g])

    def relay_y(r, side, place):
        blocks = w_scr.at[late_group(r, c), :, side]
        for j in range(1, duo):
            target = (d, 2 * lax.rem(y + j, duo) + core)
            push(blocks, blocks, yb_s.at[r, place, j - 1], yb_r.at[r, place, j - 1], target)

    def late_x(r):
        relay_x(late_group(r, c), zb_r.at[r], xb_s.at[r], xb_r.at[r])
        relay_y(r, x, 0)

    def late_y(r):
        g = late_group(r, c)
        arrived(w_scr.at[g, :, 0], xb_r.at[r])
        relay_y(r, 1 - x, 1)
        push(w_scr.at[g], w_scr.at[g], cb_s.at[r, 0], g_r.at[g], other)

    def late_core(r):
        for j in range(1, duo):
            g = late_group(r, 2 * lax.rem(y - j + duo, duo) + core)
            for place in range(2):
                arrived(w_scr.at[g, :, 0], yb_r.at[r, place, j - 1])
            push(w_scr.at[g], w_scr.at[g], cb_s.at[r, j], g_r.at[g], other)

    def late_ready(r):
        for j in range(duo):
            g = late_group(r, 2 * j + 1 - core)
            arrived(w_scr.at[g], g_r.at[g])

    def relays(todo):
        for act, r in todo:
            if r < (early_rounds if act in (early_x, early_core, early_ready) else late_rounds):
                act(r)

    with jax.named_scope('norm0'):
        normalise(0)
    with jax.named_scope('barrier'):
        pl.semaphore_wait(barrier, len(peers))
    for r in range(max(early_rounds, late_rounds)):
        if r < early_rounds:
            loads[r].wait()
            send_z(early_group(r, core), za_s.at[r], za_r.at[r])
        if r < late_rounds:
            loads[early_rounds + r].wait()
            send_z(late_group(r, c), zb_s.at[r], zb_r.at[r])
    with jax.named_scope('norm'):
        for b in range(1, batches):
            normalise(b)
    with jax.named_scope('bias'):
        bias_load.wait()
        for h in range(heads):
            bias_scr[h] = bias_scr[h].T
    with jax.named_scope('early'):
        relays([(early_x, 0), (late_x, 0), (early_core, 0), (early_x, 1)])

    def weight(g):
        value = w_scr[g]
        if rows % 16 == 0:
            return value.reshape(width, lanes)
        return value.astype(F32).reshape(width, lanes).astype(BF16)

    def project(hp):
        both = jnp.concatenate([weight(2 * hp), weight(2 * hp + 1)], axis=1)
        for b in range(batches):
            block = norm_scr[b * batch : (b + 1) * batch].reshape(batch * seq, width)
            proj = jnp.dot(block, both, preferred_element_type=F32)
            qk_scr[hp, b * batch : (b + 1) * batch] = proj.astype(BF16).reshape(batch, seq, 2 * lanes)

    def attend(hp, i):
        length = length_of(i)
        live = (col < length).astype(F32)
        q2 = qk_scr[hp, i, :, :lanes]
        k2 = qk_scr[hp, i, :, lanes:]
        logits = lax.dot_general(stack_halves(k2, low, high), q2, NT, preferred_element_type=F32)
        logits = logits.reshape(2, seq, seq) + bias_scr[pl.ds(2 * hp, 2)]
        logits = jnp.where(key < length, logits, -1e30)
        expo = jnp.exp(logits - jnp.max(logits, axis=1, keepdims=True))
        inv = live[None] / jnp.sum(expo, axis=1, keepdims=True)
        probs = (expo * inv).astype(BF16)
        p_scr[hp, i] = probs
        sums = lax.dot_general(ones, probs.reshape(2 * seq, seq), NT, preferred_element_type=F32)
        wsum_scr[hp, i, 0:1] = sums[:1, :seq]
        wsum_scr[hp, i, 1:2] = sums[:1, seq:]

    forward_plan = {
        (0, 0): [(early_ready, 0)],
        (0, 1): [(late_y, 0), (late_x, 1)],
        (1, 0): [(early_core, 1), (early_x, 2), (early_ready, 1)],
        (1, 1): [(late_x, 2)],
        (2, 0): [(late_y, 1), (late_core, 0), (late_ready, 0)],
        (2, 1): [(early_core, 2), (early_x, 3)],
        (3, 0): [(late_y, 2), (late_x, 3)],
        (3, 1): [(late_core, 1)],
        (4, 0): [(early_ready, 2), (early_core, 3)],
        (4, 1): [(late_y, 3)],
        (5, 0): [(early_ready, 3), (late_core, 2)],
    }

    def forward_step(hp, carry):
        for place in range(2):
            with jax.named_scope('fw_relay'):
                for step in range(duos):
                    todo = forward_plan.get((step, place))
                    if todo:
                        @pl.when(hp == step)
                        def _():
                            relays(todo)

            @pl.when(hp < duos)
            def _():
                with jax.named_scope('fw_block'):
                    if place == 0:
                        project(hp)
                    else:
                        for i in range(pairs):
                            attend(hp, i)

        return carry

    lax.fori_loop(0, duos, forward_step, 0)
    with jax.named_scope('late_core'):
        relays([(late_core, 3)])
    with jax.named_scope('u'):
      for i in range(pairs):
        parts = [wsum_scr[j, i] for j in range(duos)]
        if hpad > heads:
            parts.append(jnp.zeros((hpad - heads, seq), F32))
        weights = jnp.concatenate(parts, axis=0).astype(BF16)
        u_scr[i] = jnp.dot(weights, norm_scr[i], preferred_element_type=F32).astype(BF16)
    with jax.named_scope('late_ready'):
      for r in range(1, late_rounds):
        late_ready(r)

    w_v = jnp.concatenate([weight(2 * duos + j) for j in range(duos)], axis=1)
    w_o = jnp.concatenate([weight(3 * duos + j) for j in range(duos)], axis=1)
    u = u_scr[...].reshape(pairs * hpad, width)
    mixed = jnp.dot(u, w_v, preferred_element_type=F32)
    mask = head_mask(hpad, width, head_size)
    ctx32 = jnp.sum(mixed.reshape(pairs, hpad, width) * mask[None], axis=1)
    ctx = ctx32.astype(BF16)
    share = 1.0 / lengths_column(len_ref, pairs, per)
    mean = ctx32 * share
    mean_high = mean.astype(BF16)
    mean_low = (mean - mean_high.astype(F32)).astype(BF16)
    both = jnp.dot(jnp.concatenate([mean_high, mean_low], axis=0), w_o, preferred_element_type=F32)
    pooled = hsum_scr[...] * share + both[:pairs] + both[pairs:]
    factor = lax.rsqrt(jnp.mean(pooled * pooled, axis=-1, keepdims=True) + EPS)
    score = jnp.sum(pooled * factor * sw, axis=-1, keepdims=True)
    label = lengths_column(lab_ref, pairs, per)
    score = jnp.broadcast_to(score, (pairs, lanes))
    label = jnp.broadcast_to(label, (pairs, lanes))
    ex_scr[c] = jnp.concatenate([score, label], axis=0)
    for j in range(1, m):
        push(ex_scr.at[c], ex_scr.at[c], ex_s.at[j - 1], ex_r.at[j - 1], (d, lax.rem(c + j, m)))

    dot = jnp.sum(pooled * sw, axis=-1, keepdims=True) * (1.0 / width)
    slope = (factor * sw - pooled * (factor * factor * factor * dot)) * share
    cg = lax.dot_general(slope.astype(BF16), w_o, NT, preferred_element_type=F32)
    spread = (cg[:, None, :] * mask[None]).astype(BF16).reshape(pairs * hpad, width)
    wc = lax.dot_general(spread, w_v, NT, preferred_element_type=F32)
    u_scr_wc = wc.astype(BF16).reshape(pairs, hpad, width)
    for i in range(pairs):
        part = jnp.dot(u_scr_wc[i], nt_scr[:, i * seq : (i + 1) * seq], preferred_element_type=F32)
        for j in range(duos):
            dp_scr[j, i] = part[2 * j : 2 * j + 2]

    with jax.named_scope('ex_wait'):
      for j in range(1, m):
        arrived(ex_scr.at[lax.rem(c - j + m, m)], ex_r.at[j - 1])
    all_scores, all_labels = ex_scr[:, :pairs], ex_scr[:, pairs:]
    target = jnp.exp(all_labels)
    own_target = jnp.exp(label)
    query = lax.broadcasted_iota(jnp.int32, (pairs, lanes), 0) // per
    loss_row = lax.broadcasted_iota(jnp.int32, loss_ref.shape, 0)
    loss = jnp.zeros(loss_ref.shape, F32)
    score_grad = jnp.zeros((pairs, lanes), F32)

    def total(values):
        return jnp.sum(jnp.sum(values, axis=0), axis=0, keepdims=True)

    for q in range(queries):
        inside = (query == q)[None]
        highest = jnp.max(jnp.max(jnp.where(inside, all_scores, -3e38), axis=0), axis=0, keepdims=True)
        expsum = total(jnp.where(inside, jnp.exp(all_scores - highest[None]), 0.0))
        target_sum = total(jnp.where(inside, target, 0.0))
        target_dot = total(jnp.where(inside, target * all_scores, 0.0))
        loss = jnp.where(loss_row == q, highest + jnp.log(expsum) - target_dot / target_sum, loss)
        own = jnp.exp(score - highest) / expsum - own_target / target_sum
        score_grad = jnp.where(query == q, own, score_grad)
    loss_ref[...] = loss
    sg = score_grad[:, :1]
    out_grad = (slope * sg).astype(BF16)
    spread = (cg * sg).astype(BF16).astype(F32)
    spread = (spread[:, None, :] * mask[None]).astype(BF16).reshape(pairs * hpad, width)
    gv = lax.dot_general(u, spread, TN, preferred_element_type=F32).astype(BF16)
    go = lax.dot_general(ctx, out_grad, TN, preferred_element_type=F32).astype(BF16)
    for t in range(2 * duos):
        source = (gv, go)[t // duos]
        at = (t % duos) * lanes
        grads[t // 2, t % 2] = source[:, at : at + lanes].reshape(half, 2, rows, lanes)
    for i in range(pairs):
        for j in range(duos):
            dp_scr[j, i] = dp_scr[j, i] * sg[i : i + 1]

    chunks = r1.shape[0]

    def stage_core(k):
        push(grads.at[k * duo : (k + 1) * duo, 1 - core], r1.at[k], t1.at[k], v1.at[k], other)

    def stage_y(k):
        arrived(r1.at[k], v1.at[k])
        s1[k] = (grads[k * duo : (k + 1) * duo, core].astype(F32) + r1[k].astype(F32)).astype(BF16)
        for j in range(1, duo):
            peer = lax.rem(y + j, duo)
            push(s1.at[k, peer], r2.at[k, j - 1], t2.at[k, j - 1], v2.at[k, j - 1], (d, 2 * peer + core))

    def stage_x(k):
        value = s1[k, y].astype(F32)
        for j in range(1, duo):
            arrived(r2.at[k, j - 1], v2.at[k, j - 1])
            value = value + r2[k, j - 1].astype(F32)
        s2[k] = value.astype(BF16)
        push(s2.at[k, :, 1 - x], r3.at[k], t3.at[k], v3.at[k], across)

    def stage_z(k):
        arrived(r3.at[k], v3.at[k])
        s3[k] = (s2[k, :, x].astype(F32) + r3[k].astype(F32)).astype(BF16)
        for j in range(1, half):
            peer = lax.rem(z + j, half)
            push(s3.at[k, peer], r4.at[k, j - 1], t4.at[k, j - 1], v4.at[k, j - 1], (2 * peer + x, c))

    def stage_cand(k):
        value = s3[k, z].astype(F32)
        for j in range(1, half):
            arrived(r4.at[k, j - 1], v4.at[k, j - 1])
            value = value + r4[k, j - 1].astype(F32)
        fin[k * m + c] = value.astype(BF16)
        for j in range(1, m):
            piece = fin.at[k * m + c]
            push(piece, piece, t5.at[k, j - 1], v5.at[k, j - 1], (d, lax.rem(c + j, m)))

    def pair_core(k):
        push(grads.at[chunks * duo + k, 1 - core], a1.at[k], e1.at[k], f1.at[k], other)

    def pair_x(k):
        arrived(a1.at[k], f1.at[k])
        b1[k] = (grads[chunks * duo + k, core].astype(F32) + a1[k].astype(F32)).astype(BF16)
        push(b1.at[k, :, 1 - x], a2.at[k], e2.at[k], f2.at[k], across)

    def pair_z(k):
        arrived(a2.at[k], f2.at[k])
        b2[k] = (b1[k, :, x].astype(F32) + a2[k].astype(F32)).astype(BF16)
        for j in range(1, half):
            peer = lax.rem(z + j, half)
            push(b2.at[k, peer], a3.at[k, j - 1], e3.at[k, j - 1], f3.at[k, j - 1], (2 * peer + x, c))

    def pair_y(k):
        value = b2[k, z].astype(F32)
        for j in range(1, half):
            arrived(a3.at[k, j - 1], f3.at[k, j - 1])
            value = value + a3[k, j - 1].astype(F32)
        a4[k, y] = value.astype(BF16)
        for j in range(1, duo):
            target = (d, 2 * lax.rem(y + j, duo) + core)
            push(a4.at[k, y], a4.at[k, y], e4.at[k, j - 1], f4.at[k, j - 1], target)

    def pair_done(k):
        for j in range(1, duo):
            arrived(a4.at[k, lax.rem(y - j + duo, duo)], f4.at[k, j - 1])
        value = a4[k, 0].astype(F32)
        for j in range(1, duo):
            value = value + a4[k, j].astype(F32)
        piece = fin.at[2 * (chunks * duo + k) + core]
        piece[...] = value.astype(BF16)
        push(piece, piece, e5.at[k], f5.at[k], other)

    stages = (stage_core, stage_y, stage_x, stage_z, stage_cand)
    pair_stages = (pair_core, pair_x, pair_z, pair_y, pair_done)
    singles = a1.shape[0]
    blocks = 2 if pairs % 2 == 0 else 1
    size = pairs // blocks
    places = blocks + 2
    plan = []
    for k in range(chunks):
        for stage, slot in enumerate((0, 2 + k, 12 + 7 * k, 18 + 7 * k, 27 + 7 * k)):
            plan.append((slot, stage, stages[stage], k))
    for k in range(singles):
        hp = chunks * duo + k - duos
        ready = places * hp + places - 1 if hp >= 0 else 0
        for stage, slot in enumerate((0, 2, 9, 18, 22)):
            plan.append((ready + slot, 5 + stage, pair_stages[stage], k))
    plan.sort(key=lambda item: (item[0], item[1] % 5, item[3]))
    last = places * duos

    def run(hp, place):
        with jax.named_scope('bw_run'):
            for step in range(duos):
                items = [item for item in plan if item[0] == places * step + place]
                if items:
                    @pl.when(hp == step)
                    def _():
                        for _, _, act, k in items:
                            act(k)

    def differentiate(hp, i):
        probs = p_scr[hp, i].astype(F32)
        dp = dp_scr[hp, i]
        dlog = []
        for t in range(2):
            term = probs[t] * jnp.broadcast_to(dp[t : t + 1], (seq, seq)).T
            dlog.append((term - probs[t] * jnp.sum(term, axis=0, keepdims=True)).astype(BF16))
        q2 = stack_halves(qk_scr[hp, i, :, :lanes], low, high)
        k2 = stack_halves(qk_scr[hp, i, :, lanes:], low, high)
        dk = jnp.dot(jnp.concatenate(dlog, axis=1), q2, preferred_element_type=F32)
        dq = lax.dot_general(jnp.concatenate(dlog, axis=0), k2, TN, preferred_element_type=F32)
        dqk_scr[i, :, :lanes] = dq.astype(BF16)
        dqk_scr[i, :, lanes:] = dk.astype(BF16)

    def backward_step(hp, carry):
        for b in range(blocks):
            run(hp, b)

            @pl.when(hp < duos)
            def _():
                with jax.named_scope('bw_block'):
                    for j in range(size):
                        differentiate(hp, b * size + j)

        run(hp, blocks)

        @pl.when(hp < duos)
        def _():
            with jax.named_scope('bw_dot'):
                grad = jnp.dot(nt_scr[...], dqk_scr[...].reshape(pairs * seq, 2 * lanes), preferred_element_type=F32)
                grads[duos + hp, 0] = grad[:, :lanes].reshape(half, 2, rows, lanes).astype(BF16)
                grads[duos + hp, 1] = grad[:, lanes:].reshape(half, 2, rows, lanes).astype(BF16)

        run(hp, blocks + 1)
        return carry

    lax.fori_loop(0, duos, backward_step, 0)
    for slot, stage, act, k in plan:
        if slot >= last:
            with jax.named_scope('tail_%d_%d' % (stage, k)):
                act(k)
    with jax.named_scope('fin_wait'):
      for k in range(chunks):
        for j in range(1, m):
            arrived(fin.at[k * m + lax.rem(c - j + m, m)], v5.at[k, j - 1])
      for k in range(singles):
        arrived(fin.at[2 * (chunks * duo + k) + 1 - core], f5.at[k])
    part = jnp.zeros((8, lanes), F32)
    for g in range(groups):
        block = fin[g].astype(F32).reshape(rows // 8, 8, lanes)
        part = part + jnp.sum(block * block, axis=0)
    sq[...] = part
    r6[d] = part
    for j in range(1, n):
        push(sq, r6.at[d], t6.at[j - 1], v6.at[j - 1], (lax.rem(d + j, n), c))
    with jax.named_scope('sq_wait'):
      for j in range(1, n):
        arrived(r6.at[lax.rem(d - j + n, n)], v6.at[j - 1])
    count = groups * lanes * n * rows
    squares = jnp.sum(jnp.sum(jnp.sum(r6[...], axis=0), axis=0, keepdims=True), axis=1, keepdims=True)
    scale_ref[...] = jnp.broadcast_to(1.0 / (jnp.sqrt(squares / count) + EPS), scale_ref.shape)

    for a in range(early_rounds):
        arrived(w_scr.at[0, 0 : half - 1, 0], za_s.at[a])
        arrived(w_scr.at[0, :, 0], xa_s.at[a])
        arrived(w_scr.at[0], ca_s.at[a])
    for r in range(late_rounds):
        arrived(w_scr.at[0, 0 : half - 1, 0], zb_s.at[r])
        arrived(w_scr.at[0, :, 0], xb_s.at[r])
        for place in range(2):
            for j in range(duo - 1):
                arrived(w_scr.at[0, :, 0], yb_s.at[r, place, j])
        for j in range(duo):
            arrived(w_scr.at[0], cb_s.at[r, j])
    for j in range(m - 1):
        arrived(ex_scr.at[c], ex_s.at[j])
    for k in range(chunks):
        arrived(r1.at[k], t1.at[k])
        arrived(r3.at[k], t3.at[k])
        for j in range(duo - 1):
            arrived(r2.at[k, j], t2.at[k, j])
        for j in range(half - 1):
            arrived(r4.at[k, j], t4.at[k, j])
        for j in range(m - 1):
            arrived(fin.at[k * m + c], t5.at[k, j])
    for k in range(singles):
        arrived(a1.at[k], e1.at[k])
        arrived(a2.at[k], e2.at[k])
        for j in range(half - 1):
            arrived(a3.at[k, j], e3.at[k, j])
        for j in range(duo - 1):
            arrived(a4.at[k, 0], e4.at[k, j])
        arrived(fin.at[0], e5.at[k])
    for j in range(n - 1):
        arrived(sq, t6.at[j])


def finish_kernel(duos, fin, scale_ref, loss_in, out_ref, loss_ref):
    groups, rows, lanes = fin.shape
    scale = scale_ref[0:1, :]
    for at in range(groups):
        if at < 2 * duos:
            col = 2 * duos + at
        else:
            col = (at % 2) * duos + (at - 2 * duos) // 2
        out_ref[:, col * lanes : (col + 1) * lanes] = fin[at].astype(F32) * scale
    for q in range(loss_ref.shape[0]):
        loss_ref[q] = jnp.max(loss_in[q : q + 1, :])


def shards(hidden, attn_weight, norm_gain, pos_bias, score_weight, pair_lengths, labels):
    queries, per, seq, width = hidden.shape
    pairs = queries * per
    heads = pos_bias.shape[0]
    n, m = lax.axis_size("dp"), lax.axis_size("cand")
    lanes = 2 * (width // heads)
    duos = heads // 2
    groups = 4 * duos
    rows, half, duo = width // n, n // 2, m // 2
    early = groups // 3
    early_rounds, late_rounds = early // 2, (groups - early) // m
    batch = 4 if pairs % 4 == 0 else 1
    hpad = -(-heads // 16) * 16
    chunks = duos // duo
    singles = 2 * duos - chunks * duo
    near, far = max(duo - 1, 1), max(half - 1, 1)
    dma = pltpu.SemaphoreType.DMA
    vmem = pltpu.VMEM
    here = pl.BlockSpec(memory_space=pltpu.VMEM)
    away = pl.BlockSpec(memory_space=pl.ANY)
    small = pl.BlockSpec(memory_space=pltpu.SMEM)
    loss_rows = -(-queries // 8) * 8
    fin, scale, loss = pl.pallas_call(
        functools.partial(fused_kernel, n, m, early),
        in_specs=[small, small, away, away, here, away, here],
        out_specs=[here, here, here],
        out_shape=[
            jax.ShapeDtypeStruct((groups, rows, lanes), BF16),
            jax.ShapeDtypeStruct((8, lanes), F32),
            jax.ShapeDtypeStruct((loss_rows, lanes), F32),
        ],
        scratch_shapes=[
            vmem((pairs, seq, width), BF16),
            vmem(pos_bias.shape, F32),
            vmem((groups, half, 2, rows, lanes), BF16),
            vmem((pairs, seq, width), BF16),
            vmem((width, pairs * seq), BF16),
            vmem((duos, pairs, seq, 2 * lanes), BF16),
            vmem((duos, pairs, 2, seq, seq), BF16),
            vmem((duos, pairs, 2, seq), F32),
            vmem((pairs, hpad, width), BF16),
            vmem((pairs, width), F32),
            vmem((m, 2 * pairs, lanes), F32),
            vmem((duos, pairs, 2, seq), F32),
            vmem((pairs, seq, 2 * lanes), BF16),
            vmem((2 * duos, 2, half, 2, rows, lanes), BF16),
            vmem((chunks, duo, half, 2, rows, lanes), BF16),
            vmem((chunks, duo, half, 2, rows, lanes), BF16),
            vmem((chunks, near, half, 2, rows, lanes), BF16),
            vmem((chunks, half, 2, rows, lanes), BF16),
            vmem((chunks, half, rows, lanes), BF16),
            vmem((chunks, half, rows, lanes), BF16),
            vmem((chunks, far, rows, lanes), BF16),
            vmem((singles, half, 2, rows, lanes), BF16),
            vmem((singles, half, 2, rows, lanes), BF16),
            vmem((singles, half, rows, lanes), BF16),
            vmem((singles, half, rows, lanes), BF16),
            vmem((singles, far, rows, lanes), BF16),
            vmem((singles, duo, rows, lanes), BF16),
            vmem((8, lanes), F32),
            vmem((n, 8, lanes), F32),
            dma((pairs // batch,)), dma, dma((early_rounds,)), dma((late_rounds,)),
            dma((early_rounds,)), dma((early_rounds,)), dma((early_rounds,)), dma((early_rounds,)),
            dma((early_rounds,)),
            dma((late_rounds,)), dma((late_rounds,)), dma((late_rounds,)), dma((late_rounds,)),
            dma((late_rounds, 2, near)), dma((late_rounds, 2, near)), dma((late_rounds, duo)), dma((groups,)),
            dma((m - 1,)), dma((m - 1,)),
            dma((chunks,)), dma((chunks,)),
            dma((chunks, near)), dma((chunks, near)),
            dma((chunks,)), dma((chunks,)),
            dma((chunks, far)), dma((chunks, far)),
            dma((chunks, m - 1)), dma((chunks, m - 1)),
            dma((n - 1,)), dma((n - 1,)),
            dma((singles,)), dma((singles,)),
            dma((singles,)), dma((singles,)),
            dma((singles, far)), dma((singles, far)),
            dma((singles, near)), dma((singles, near)),
            dma((singles,)), dma((singles,)),
        ],
        compiler_params=pltpu.CompilerParams(
            collective_id=0, has_side_effects=True, vmem_limit_bytes=VMEM_LIMIT
        ),
        name="fused_step",
    )(pair_lengths, labels, hidden.reshape(pairs, seq, width), attn_weight, norm_gain, pos_bias, score_weight)
    update, loss = pl.pallas_call(
        functools.partial(finish_kernel, duos),
        in_specs=[here, here, here],
        out_specs=[here, small],
        out_shape=[
            jax.ShapeDtypeStruct((rows, 4 * width), F32),
            jax.ShapeDtypeStruct((queries,), F32),
        ],
        name="finish",
    )(fin, scale, loss)
    return (update, loss)


def solution(mesh):
    in_specs = (
        P("dp", "cand", None, None),
        P("dp", None),
        P(),
        P(),
        P(),
        P("dp", "cand"),
        P("dp", "cand"),
    )
    out_specs = (P("dp", None), P("dp"))
    return jax.shard_map(shards, mesh=mesh, in_specs=in_specs, out_specs=out_specs, check_vma=False)
```

```python
import functools

import jax
import jax.numpy as jnp
from jax import lax
from jax.experimental import pallas as pl
from jax.experimental.pallas import tpu as pltpu
from jax.sharding import PartitionSpec as P

EPS = 1e-06
F32 = jnp.float32
BF16 = jnp.bfloat16
VMEM_LIMIT = 60 * 1024 * 1024
LEAD = 4
NT = (((1,), (1,)), ((), ()))
TN = (((0,), (0,)), ((), ()))
MESH = pl.DeviceIdType.MESH


def half_masks(lanes):
    lane = lax.broadcasted_iota(jnp.int32, (1, lanes), 1)
    low = (lane < lanes // 2).astype(F32)
    return low.astype(BF16), (1.0 - low).astype(BF16)


def stack_halves(block, low, high):
    return jnp.concatenate([block * low, block * high], axis=0)


def head_mask(hpad, width, head_size):
    lane = lax.broadcasted_iota(jnp.int32, (hpad, width), 1)
    head = lax.broadcasted_iota(jnp.int32, (hpad, width), 0)
    start = head * head_size
    return ((lane >= start) & (lane < start + head_size)).astype(F32)


def arrived(ref, sem):
    pltpu.make_async_copy(ref, ref, sem).wait()


def push(src, dst, send, recv, target):
    pltpu.make_async_remote_copy(
        src_ref=src, dst_ref=dst, send_sem=send, recv_sem=recv, device_id=target, device_id_type=MESH
    ).start()


def lengths_column(ref, pairs, per):
    row = lax.broadcasted_iota(jnp.int32, (pairs, 1), 0)
    column = jnp.zeros((pairs, 1), F32)
    for i in range(pairs):
        column = jnp.where(row == i, ref[i // per, i % per].astype(F32), column)
    return column


def fused_kernel(n, m, early, len_ref, lab_ref, h_hbm, w_hbm, gain_ref, bias_hbm, sw_ref,
                 fin_hbm, loss_ref,
                 fin, h_scr, bias_scr, w_scr, norm_scr, nt_scr, qk_scr, p_scr, wsum_scr, u_scr, hsum_scr, ex_scr,
                 dp_scr, dqk_scr, grads, r1, s1, r2, s2, r3, s3, r4, a1, b1, a2, b2, a3, a4, sq, r6,
                 h_sem, b_sem, wa_sem, wb_sem,
                 za_r, xa_r, zb_r, xb_r, yb_r, ga_r, gb_r, few_s, many_s, ex_s, ex_r,
                 t1, v1, t2, v2, t3, v3, t4, v4, t5, v5, t6, v6,
                 e1, f1, e2, f2, e3, f3, e4, f4, e5, f5):
    pairs, seq, width = h_scr.shape
    queries, per = len_ref.shape
    heads = bias_scr.shape[0]
    groups, half, _, rows, lanes = w_scr.shape
    duos = heads // 2
    duo = m // 2
    head_size = width // heads
    hpad = u_scr.shape[1]
    batch = pairs // h_sem.shape[0]
    batches = pairs // batch
    early_rounds = early // 2
    late_rounds = (groups - early) // m
    d, c = lax.axis_index("dp"), lax.axis_index("cand")
    z, x = d // 2, d % 2
    y, core = c // 2, c % 2
    across = (d + 1 - 2 * x, c)
    other = (d, c + 1 - 2 * core)

    lead = LEAD

    def column(g):
        tail = g // (2 * duos)
        return (1 - tail) * (g // 2 + (g % 2) * duos) + tail * g

    early_slots = (0, duos, groups - 4, groups - 2)

    def early_group(a, which):
        return early_slots[a] + which

    def late_group(r, which):
        if r == 0:
            return 2 + which + 2 * (which // 4)
        return 4 + r * m + which

    order = [("late", 0), ("early", 0), ("late", 1), ("early", 1), ("late", 2), ("early", 2), ("late", 3), ("early", 3)]
    order = [(kind, r) for kind, r in order if kind == "early" or r < late_rounds]

    def load(g, sem):
        at = pl.multiple_of(column(g) * lanes, lanes)
        return pltpu.make_async_copy(w_hbm.at[:, pl.ds(at, lanes)], w_scr.at[g, z, x], sem)

    loads = [load(early_group(a, core), wa_sem.at[a]) for a in range(early_rounds)]
    loads += [load(late_group(r, c), wb_sem.at[r, 0]) for r in range(late_rounds)]
    mirrors = [
        [load(late_group(r, 2 * lax.rem(y - j + duo, duo) + core), wb_sem.at[r, j]) for j in range(1, duo)]
        for r in range(late_rounds)
    ]
    tokens = []
    for b in range(batches):
        part = pl.ds(b * batch, batch)
        tokens.append(pltpu.make_async_copy(h_hbm.at[part], h_scr.at[part], h_sem.at[b]))
    bias_load = pltpu.make_async_copy(bias_hbm, bias_scr, b_sem)
    for copy in loads + tokens + [bias_load] + sum(mirrors, []):
        copy.start()
    peers = [(d, lax.rem(c + j, m)) for j in range(1, m)] + [(lax.rem(d + j, n), c) for j in range(1, n)]
    peers += [(lax.rem(d + j, n), other[1]) for j in range(1, n)]
    barrier = pltpu.get_barrier_semaphore()
    for peer in peers:
        pl.semaphore_signal(barrier, inc=1, device_id=peer, device_id_type=MESH)

    col = lax.broadcasted_iota(jnp.int32, (1, seq), 1)
    row = lax.broadcasted_iota(jnp.int32, (seq, 1), 0)
    key = lax.broadcasted_iota(jnp.int32, (2, seq, seq), 1)
    low, high = half_masks(lanes)
    gain = gain_ref[...].reshape(1, width)
    sw = sw_ref[...].reshape(1, width)

    def length_of(i):
        return len_ref[i // per, i % per]

    def normalise(b):
        tokens[b].wait()
        values = h_scr[b * batch : (b + 1) * batch].reshape(batch * seq, width).astype(F32)
        factor = lax.rsqrt(jnp.mean(values * values, axis=-1, keepdims=True) + EPS)
        normed = (values * factor * gain).astype(BF16)
        norm_scr[b * batch : (b + 1) * batch] = normed.reshape(batch, seq, width)
        nt_scr[:, b * batch * seq : (b + 1) * batch * seq] = normed.T
        for j in range(batch):
            i = b * batch + j
            live = (row < length_of(i)).astype(F32)
            hsum_scr[i : i + 1, :] = jnp.sum(values[j * seq : (j + 1) * seq] * live, axis=0, keepdims=True)

    hops = [1] + [half - 1] * (half > 2) + list(range(2, half - 1))

    def send_z(g, s, r, x_s, x_r):
        block = w_scr.at[g, z, x]
        for j in hops:
            push(block, block, s, r.at[j - 1], (2 * lax.rem(z + j, half) + x, c))
        push(block, block, x_s, x_r, across)

    def relay_x(g, z_sem, s, r, also=None):
        for j in hops:
            block = w_scr.at[g, lax.rem(z - j + half, half), x]
            arrived(block, z_sem.at[j - 1])
            push(block, block, s, r, across)
            if also is not None:
                relay_y(block, also, 0)

    def send_round(i):
        if i >= len(order):
            return
        kind, r = order[i]
        if kind == "early":
            loads[r].wait()
            send_z(early_group(r, core), few_s, za_r.at[r], many_s, xa_r.at[r])
        else:
            loads[early_rounds + r].wait()
            send_z(late_group(r, c), few_s, zb_r.at[r], many_s, xb_r.at[r])

    def early_x(a):
        relay_x(early_group(a, core), za_r.at[a], many_s, xa_r.at[a])
        send_round(order.index(("early", a)) + lead)

    def early_core(a):
        g = early_group(a, core)
        arrived(w_scr.at[g, :, 0], xa_r.at[a])
        push(w_scr.at[g], w_scr.at[g], many_s, ga_r.at[a], other)

    def early_ready(a):
        g = early_group(a, 1 - core)
        arrived(w_scr.at[g], ga_r.at[a])

    def relay_y(blocks, r, place):
        for j in range(1, duo):
            target = (d, 2 * lax.rem(y + j, duo) + core)
            push(blocks, blocks, (few_s, many_s)[place], yb_r.at[r, place, j - 1], target)

    def late_x(r):
        relay_x(late_group(r, c), zb_r.at[r], many_s, xb_r.at[r], r)
        send_round(order.index(("late", r)) + lead)

    def late_y(r):
        g = late_group(r, c)
        arrived(w_scr.at[g, :, 0], xb_r.at[r])
        relay_y(w_scr.at[g, :, 1 - x], r, 1)
        push(w_scr.at[g], w_scr.at[g], many_s, gb_r.at[r], other)

    def late_core(r):
        for j in range(1, duo):
            g = late_group(r, 2 * lax.rem(y - j + duo, duo) + core)
            mirrors[r][j - 1].wait()
            arrived(w_scr.at[g, 0 : half - 1, 0], yb_r.at[r, 0, j - 1])
            arrived(w_scr.at[g, :, 0], yb_r.at[r, 1, j - 1])
            push(w_scr.at[g], w_scr.at[g], many_s, gb_r.at[r], other)

    def late_ready(r):
        arrived(w_scr.at[0:duo], gb_r.at[r])

    def relays(todo):
        for act, r in todo:
            if r < (early_rounds if act in (early_x, early_core, early_ready) else late_rounds):
                with jax.named_scope(act.__name__ + '_%d' % r):
                    act(r)

    with jax.named_scope('norm0'):
        normalise(0)
    with jax.named_scope('barrier'):
        pl.semaphore_wait(barrier, len(peers))
    for i in range(lead):
        send_round(i)
    with jax.named_scope('norm'):
        for b in range(1, batches):
            normalise(b)
    with jax.named_scope('bias'):
        bias_load.wait()
        for h in range(heads):
            bias_scr[h] = bias_scr[h].T
    with jax.named_scope('early'):
        relays([(late_x, 0), (early_x, 0), (late_y, 0), (late_x, 1), (early_core, 0), (early_ready, 0)])

    def weight(g):
        value = w_scr[g]
        if rows % 16 == 0:
            return value.reshape(width, lanes)
        return value.astype(F32).reshape(width, lanes).astype(BF16)

    def project(hp):
        both = jnp.concatenate([weight(2 * hp), weight(2 * hp + 1)], axis=1)
        for b in range(batches):
            block = norm_scr[b * batch : (b + 1) * batch].reshape(batch * seq, width)
            proj = jnp.dot(block, both, preferred_element_type=F32)
            qk_scr[hp, b * batch : (b + 1) * batch] = proj.astype(BF16).reshape(batch, seq, 2 * lanes)

    def attend(hp, i):
        length = length_of(i)
        live = (col < length).astype(F32)
        q2 = qk_scr[hp, i, :, :lanes]
        k2 = qk_scr[hp, i, :, lanes:]
        logits = lax.dot_general(stack_halves(k2, low, high), q2, NT, preferred_element_type=F32)
        logits = logits.reshape(2, seq, seq) + bias_scr[pl.ds(2 * hp, 2)]
        logits = jnp.where(key < length, logits, -1e30)
        expo = jnp.exp(logits - jnp.max(logits, axis=1, keepdims=True))
        inv = live[None] / jnp.sum(expo, axis=1, keepdims=True)
        probs = (expo * inv).astype(BF16)
        probs = jnp.stack([probs[0].T, probs[1].T])
        p_scr[hp, i] = probs
        wsum_scr[hp, i] = jnp.sum(probs.astype(F32), axis=1)

    forward_plan = {
        (0, 1): [(early_x, 1), (late_core, 0), (late_y, 1), (late_x, 2)],
        (1, 0): [(late_ready, 0)],
        (1, 1): [(early_core, 1), (early_x, 2)],
        (2, 1): [(late_y, 2), (late_core, 1), (late_x, 3)],
        (3, 0): [(early_ready, 1)],
        (3, 1): [(early_core, 2), (early_x, 3)],
        (4, 0): [(late_ready, 1), (late_y, 3)],
        (4, 1): [(late_core, 2)],
        (5, 0): [(early_core, 3)],
    }

    def forward_step(hp, carry):
        for place in range(2):
            with jax.named_scope('fw_relay'):
                for step in range(duos):
                    todo = forward_plan.get((step, place))
                    if todo:
                        @pl.when(hp == step)
                        def _():
                            relays(todo)

            @pl.when(hp < duos)
            def _():
                with jax.named_scope('fw_block'):
                    if place == 0:
                        project(hp)
                    else:
                        for i in range(pairs):
                            attend(hp, i)

        return carry

    lax.fori_loop(0, duos, forward_step, 0)
    with jax.named_scope('late_core'):
        relays([(late_core, 3)])
    with jax.named_scope('u'):
      for i in range(pairs):
        parts = [wsum_scr[j, i] for j in range(duos)]
        if hpad > heads:
            parts.append(jnp.zeros((hpad - heads, seq), F32))
        weights = jnp.concatenate(parts, axis=0).astype(BF16)
        u_scr[i] = jnp.dot(weights, norm_scr[i], preferred_element_type=F32).astype(BF16)
    with jax.named_scope('late_ready'):
      relays([(late_ready, 2), (late_ready, 3), (early_ready, 2), (early_ready, 3)])

    w_v = jnp.concatenate([weight(2 * duos + j) for j in range(duos)], axis=1)
    w_o = jnp.concatenate([weight(3 * duos + j) for j in range(duos)], axis=1)
    u = u_scr[...].reshape(pairs * hpad, width)
    mixed = jnp.dot(u, w_v, preferred_element_type=F32)
    mask = head_mask(hpad, width, head_size)
    ctx32 = jnp.sum(mixed.reshape(pairs, hpad, width) * mask[None], axis=1)
    ctx = ctx32.astype(BF16)
    share = 1.0 / lengths_column(len_ref, pairs, per)
    mean = ctx32 * share
    mean_high = mean.astype(BF16)
    mean_low = (mean - mean_high.astype(F32)).astype(BF16)
    both = jnp.dot(jnp.concatenate([mean_high, mean_low], axis=0), w_o, preferred_element_type=F32)
    pooled = hsum_scr[...] * share + both[:pairs] + both[pairs:]
    factor = lax.rsqrt(jnp.mean(pooled * pooled, axis=-1, keepdims=True) + EPS)
    score = jnp.sum(pooled * factor * sw, axis=-1, keepdims=True)
    label = lengths_column(lab_ref, pairs, per)
    score = jnp.broadcast_to(score, (pairs, lanes))
    label = jnp.broadcast_to(label, (pairs, lanes))
    ex_scr[c] = jnp.concatenate([score, label], axis=0)
    for j in range(1, m):
        push(ex_scr.at[c], ex_scr.at[c], ex_s, ex_r, (d, lax.rem(c + j, m)))

    dot = jnp.sum(pooled * sw, axis=-1, keepdims=True) * (1.0 / width)
    slope = (factor * sw - pooled * (factor * factor * factor * dot)) * share
    cg = lax.dot_general(slope.astype(BF16), w_o, NT, preferred_element_type=F32)
    spread = (cg[:, None, :] * mask[None]).astype(BF16).reshape(pairs * hpad, width)
    wc = lax.dot_general(spread, w_v, NT, preferred_element_type=F32)
    u_scr_wc = wc.astype(BF16).reshape(pairs, hpad, width)
    for i in range(pairs):
        part = jnp.dot(u_scr_wc[i], nt_scr[:, i * seq : (i + 1) * seq], preferred_element_type=F32)
        for j in range(duos):
            dp_scr[j, i] = part[2 * j : 2 * j + 2]

    with jax.named_scope('ex_wait'):
      arrived(ex_scr.at[0 : m - 1], ex_r)
    all_scores, all_labels = ex_scr[:, :pairs], ex_scr[:, pairs:]
    target = jnp.exp(all_labels)
    own_target = jnp.exp(label)
    query = lax.broadcasted_iota(jnp.int32, (pairs, lanes), 0) // per
    loss_row = lax.broadcasted_iota(jnp.int32, loss_ref.shape, 0)
    loss = jnp.zeros(loss_ref.shape, F32)
    score_grad = jnp.zeros((pairs, lanes), F32)

    def total(values):
        return jnp.sum(jnp.sum(values, axis=0), axis=0, keepdims=True)

    for q in range(queries):
        inside = (query == q)[None]
        highest = jnp.max(jnp.max(jnp.where(inside, all_scores, -3e38), axis=0), axis=0, keepdims=True)
        expsum = total(jnp.where(inside, jnp.exp(all_scores - highest[None]), 0.0))
        target_sum = total(jnp.where(inside, target, 0.0))
        target_dot = total(jnp.where(inside, target * all_scores, 0.0))
        loss = jnp.where(loss_row == q + 1, highest + jnp.log(expsum) - target_dot / target_sum, loss)
        own = jnp.exp(score - highest) / expsum - own_target / target_sum
        score_grad = jnp.where(query == q, own, score_grad)
    loss_ref[...] = loss
    sg = score_grad[:, :1]
    out_grad = (slope * sg).astype(BF16)
    spread = (cg * sg).astype(BF16).astype(F32)
    spread = (spread[:, None, :] * mask[None]).astype(BF16).reshape(pairs * hpad, width)
    gv = lax.dot_general(u, spread, TN, preferred_element_type=F32).astype(BF16)
    go = lax.dot_general(ctx, out_grad, TN, preferred_element_type=F32).astype(BF16)
    for t in range(2 * duos):
        source = (gv, go)[t // duos]
        at = (t % duos) * lanes
        grads[t // 2, t % 2] = source[:, at : at + lanes].reshape(half, 2, rows, lanes)
    for i in range(pairs):
        for j in range(duos):
            dp_scr[j, i] = dp_scr[j, i] * sg[i : i + 1]

    chunks = r1.shape[0]

    def finish_chunks(part, waiting, square):
        with jax.named_scope('chunk_wait'):
            if waiting:
                arrived(fin.at[0 : len(waiting) * (m - 1)], v5)
            for g in range(len(waiting) * m):
                part = part + square(g)
        return part

    def stage_core(k):
        push(grads.at[k * duo : (k + 1) * duo, 1 - core], r1.at[k], t1, v1.at[k], other)

    def stage_y(k):
        arrived(r1.at[k], v1.at[k])
        s1[k] = (grads[k * duo : (k + 1) * duo, core].astype(F32) + r1[k].astype(F32)).astype(BF16)
        for j in range(1, duo):
            peer = lax.rem(y + j, duo)
            push(s1.at[k, peer], r2.at[k, j - 1], t2, v2.at[k], (d, 2 * peer + core))

    def stage_x(k):
        value = s1[k, y].astype(F32)
        if duo > 1:
            arrived(r2.at[k], v2.at[k])
        for j in range(1, duo):
            value = value + r2[k, j - 1].astype(F32)
        s2[k] = value.astype(BF16)
        push(s2.at[k, :, 1 - x], r3.at[k], t3, v3.at[k], across)

    def stage_z(k):
        arrived(r3.at[k], v3.at[k])
        s3[k] = (s2[k, :, x].astype(F32) + r3[k].astype(F32)).astype(BF16)
        for j in range(1, half):
            peer = lax.rem(z + j, half)
            push(s3.at[k, peer], r4.at[k, j - 1], t4, v4.at[k], (2 * peer + x, c))

    def stage_cand(k):
        value = s3[k, z].astype(F32)
        if half > 1:
            arrived(r4.at[k], v4.at[k])
        for j in range(1, half):
            value = value + r4[k, j - 1].astype(F32)
        fin[k * m + c] = value.astype(BF16)
        for j in range(1, m):
            piece = fin.at[k * m + c]
            push(piece, piece, t5, v5, (d, lax.rem(c + j, m)))

    def pair_core(k):
        push(grads.at[chunks * duo + k, 1 - core], a1.at[k], e1, f1.at[k], other)

    def pair_x(k):
        arrived(a1.at[k], f1.at[k])
        b1[k] = (grads[chunks * duo + k, core].astype(F32) + a1[k].astype(F32)).astype(BF16)
        push(b1.at[k, :, 1 - x], a2.at[k], e2, f2.at[k], across)

    def pair_z(k):
        arrived(a2.at[k], f2.at[k])
        b2[k] = (b1[k, :, x].astype(F32) + a2[k].astype(F32)).astype(BF16)
        for j in range(1, half):
            peer = lax.rem(z + j, half)
            push(b2.at[k, peer], a3.at[k, j - 1], e3, f3.at[k], (2 * peer + x, c))

    def pair_y(k):
        value = b2[k, z].astype(F32)
        if half > 1:
            arrived(a3.at[k], f3.at[k])
        for j in range(1, half):
            value = value + a3[k, j - 1].astype(F32)
        a4[k, y] = value.astype(BF16)
        for j in range(1, duo):
            target = (d, 2 * lax.rem(y + j, duo) + core)
            push(a4.at[k, y], a4.at[k, y], e4, f4.at[k], target)

    def pair_done(k):
        if duo > 1:
            arrived(a4.at[k, 0 : duo - 1], f4.at[k])
        value = a4[k, 0].astype(F32)
        for j in range(1, duo):
            value = value + a4[k, j].astype(F32)
        piece = fin.at[2 * (chunks * duo + k) + core]
        piece[...] = value.astype(BF16)
        push(piece, piece, e5, f5, other)

    stages = (stage_core, stage_y, stage_x, stage_z, stage_cand)
    pair_stages = (pair_core, pair_x, pair_z, pair_y, pair_done)
    singles = a1.shape[0]
    step_time = 2.25
    plan = []
    for k in range(chunks):
        for stage, at in enumerate((0.0, 1.3 + 0.5 * k, 7.7 + 4.2 * k, 12.4 + 4.2 * k, 18.0 + 4.2 * k)):
            plan.append((at, stage, stages[stage], k))
    for k in range(singles):
        hp = chunks * duo + k - duos
        ready = step_time * (hp + 1) - 0.05 if hp >= 0 else 0.0
        for stage, at in enumerate((0.0, 1.2, 5.6, 11.0, 14.0)):
            plan.append((ready + at, 5 + stage, pair_stages[stage], k))
    plan.sort(key=lambda item: (item[0], item[1] % 5, item[3]))
    slots = [(step_time * hp + at, hp, place) for hp in range(duos)
             for place, at in enumerate((0.0, 1.3, step_time - 0.05))]
    homes = {}
    for item in plan:
        home = next(((hp, place) for at, hp, place in slots if at >= item[0] - 0.1), None)
        homes.setdefault(home, []).append(item)

    def run(hp, place):
        with jax.named_scope('bw_run'):
            for step in range(duos):
                items = homes.get((step, place))
                if items:
                    @pl.when(hp == step)
                    def _():
                        for _, stage, act, k in items:
                            with jax.named_scope('in_%d_%d' % (stage, k)):
                                act(k)

    def differentiate(hp, i):
        probs = p_scr[hp, i].astype(F32)
        term = probs * dp_scr[hp, i][:, None, :]
        dlog = (term - probs * jnp.sum(term, axis=-1, keepdims=True)).astype(BF16)
        wide = jnp.concatenate([dlog[0], dlog[1]], axis=1)
        q2 = stack_halves(qk_scr[hp, i, :, :lanes], low, high)
        k2 = stack_halves(qk_scr[hp, i, :, lanes:], low, high)
        dq = jnp.dot(wide, k2, preferred_element_type=F32)
        dk = lax.dot_general(dlog.reshape(2 * seq, seq), q2, TN, preferred_element_type=F32)
        dqk_scr[i, :, :lanes] = dq.astype(BF16)
        dqk_scr[i, :, lanes:] = dk.astype(BF16)

    def backward_step(hp, carry):
        run(hp, 0)

        @pl.when(hp < duos)
        def _():
            with jax.named_scope('bw_block'):
                for i in range(pairs):
                    differentiate(hp, i)

        run(hp, 1)

        @pl.when(hp < duos)
        def _():
            with jax.named_scope('bw_dot'):
                grad = jnp.dot(nt_scr[...], dqk_scr[...].reshape(pairs * seq, 2 * lanes), preferred_element_type=F32)
                grads[duos + hp, 0] = grad[:, :lanes].reshape(half, 2, rows, lanes).astype(BF16)
                grads[duos + hp, 1] = grad[:, lanes:].reshape(half, 2, rows, lanes).astype(BF16)

        run(hp, 2)
        return carry

    lax.fori_loop(0, duos, backward_step, 0)
    def square(g):
        block = fin[g].astype(F32).reshape(rows // 8, 8, lanes)
        return jnp.sum(block * block, axis=0)

    part = jnp.zeros((8, lanes), F32)
    waiting = [k for k in range(chunks)]
    for _, stage, act, k in homes.get(None, []):
        if stage == 9 and waiting and k == singles - 1:
            part = finish_chunks(part, waiting, square)
            waiting = []
        with jax.named_scope('tail_%d_%d' % (stage, k)):
            act(k)
    if waiting:
        part = finish_chunks(part, waiting, square)
    part = jnp.where(core == 0, part, 0.0)
    for k in range(singles):
        part = part + square(2 * (chunks * duo + k) + core)
    sq[...] = part
    mine = core * n + d
    r6[mine] = part
    targets = [(lax.rem(d + j, n), core) for j in range(1, n)] + [(lax.rem(d + j, n), 1 - core) for j in range(n)]
    for t, (to, to_core) in enumerate(targets):
        push(sq, r6.at[mine], t6, v6, (to, c - core + to_core))
    with jax.named_scope('fin_wait'):
        arrived(fin.at[0:singles], f5)
    store = pltpu.make_async_copy(fin, fin_hbm, b_sem)
    store.start()
    with jax.named_scope('drain'):
        kinds = early_rounds + late_rounds * duo
        arrived(w_scr.at[0:kinds, 0 : half - 1, 0], few_s)
        arrived(w_scr.at[0 : 3 * kinds // 2], many_s)
        arrived(ex_scr.at[0 : m - 1], ex_s)
        if chunks:
            arrived(r1, t1)
            arrived(r3, t3)
            arrived(fin.at[0 : chunks * (m - 1)], t5)
            if duo > 1:
                arrived(r2, t2)
            if half > 1:
                arrived(r4, t4)
        arrived(a1, e1)
        arrived(a2, e2)
        arrived(fin.at[0:singles], e5)
        if half > 1:
            arrived(a3, e3)
        if duo > 1:
            arrived(a4.at[:, 0 : duo - 1], e4)
    with jax.named_scope('sq_wait'):
        arrived(r6.at[0 : 2 * n - 1], v6)
        arrived(r6.at[0 : 2 * n - 1], t6)
    count = groups * lanes * n * rows
    squares = jnp.sum(r6[...], axis=0)
    squares = jnp.sum(jnp.sum(squares, axis=0, keepdims=True), axis=1, keepdims=True)
    loss_ref[0:1, :] = jnp.broadcast_to(1.0 / (jnp.sqrt(squares / count) + EPS), (1, lanes))
    store.wait()


def finish_kernel(duos, fin, loss_in, out_ref, loss_ref):
    groups, rows, lanes = fin.shape
    scale = loss_in[0:1, :]
    for at in range(groups):
        if at < 2 * duos:
            col = 2 * duos + at
        else:
            col = (at % 2) * duos + (at - 2 * duos) // 2
        out_ref[:, col * lanes : (col + 1) * lanes] = fin[at].astype(F32) * scale
    for q in range(loss_ref.shape[0]):
        loss_ref[q] = jnp.max(loss_in[q + 1 : q + 2, :])


def shards(hidden, attn_weight, norm_gain, pos_bias, score_weight, pair_lengths, labels):
    queries, per, seq, width = hidden.shape
    pairs = queries * per
    heads = pos_bias.shape[0]
    n, m = lax.axis_size("dp"), lax.axis_size("cand")
    lanes = 2 * (width // heads)
    duos = heads // 2
    groups = 4 * duos
    rows, half, duo = width // n, n // 2, m // 2
    early = groups // 3
    early_rounds, late_rounds = early // 2, (groups - early) // m
    batch = 4 if pairs % 4 == 0 else 1
    hpad = -(-heads // 16) * 16
    chunks = max(duos // duo - 1, 1)
    singles = 2 * duos - chunks * duo
    near, far = max(duo - 1, 1), max(half - 1, 1)
    dma = pltpu.SemaphoreType.DMA
    vmem = pltpu.VMEM
    here = pl.BlockSpec(memory_space=pltpu.VMEM)
    away = pl.BlockSpec(memory_space=pl.ANY)
    small = pl.BlockSpec(memory_space=pltpu.SMEM)
    loss_rows = -(-(queries + 1) // 8) * 8
    fin, loss = pl.pallas_call(
        functools.partial(fused_kernel, n, m, early),
        in_specs=[small, small, away, away, here, away, here],
        out_specs=[away, here],
        out_shape=[
            jax.ShapeDtypeStruct((groups, rows, lanes), BF16),
            jax.ShapeDtypeStruct((loss_rows, lanes), F32),
        ],
        scratch_shapes=[
            vmem((groups, rows, lanes), BF16),
            vmem((pairs, seq, width), BF16),
            vmem(pos_bias.shape, F32),
            vmem((groups, half, 2, rows, lanes), BF16),
            vmem((pairs, seq, width), BF16),
            vmem((width, pairs * seq), BF16),
            vmem((duos, pairs, seq, 2 * lanes), BF16),
            vmem((duos, pairs, 2, seq, seq), BF16),
            vmem((duos, pairs, 2, seq), F32),
            vmem((pairs, hpad, width), BF16),
            vmem((pairs, width), F32),
            vmem((m, 2 * pairs, lanes), F32),
            vmem((duos, pairs, 2, seq), F32),
            vmem((pairs, seq, 2 * lanes), BF16),
            vmem((2 * duos, 2, half, 2, rows, lanes), BF16),
            vmem((chunks, duo, half, 2, rows, lanes), BF16),
            vmem((chunks, duo, half, 2, rows, lanes), BF16),
            vmem((chunks, near, half, 2, rows, lanes), BF16),
            vmem((chunks, half, 2, rows, lanes), BF16),
            vmem((chunks, half, rows, lanes), BF16),
            vmem((chunks, half, rows, lanes), BF16),
            vmem((chunks, far, rows, lanes), BF16),
            vmem((singles, half, 2, rows, lanes), BF16),
            vmem((singles, half, 2, rows, lanes), BF16),
            vmem((singles, half, rows, lanes), BF16),
            vmem((singles, half, rows, lanes), BF16),
            vmem((singles, far, rows, lanes), BF16),
            vmem((singles, duo, rows, lanes), BF16),
            vmem((8, lanes), F32),
            vmem((2 * n, 8, lanes), F32),
            dma((pairs // batch,)), dma, dma((early_rounds,)), dma((late_rounds, duo)),
            dma((early_rounds, far)), dma((early_rounds,)), dma((late_rounds, far)), dma((late_rounds,)),
            dma((late_rounds, 2, near)), dma((early_rounds,)), dma((late_rounds,)), dma, dma, dma, dma,
            dma, dma((chunks,)), dma, dma((chunks,)), dma, dma((chunks,)), dma, dma((chunks,)), dma, dma, dma, dma,
            dma, dma((singles,)), dma, dma((singles,)), dma, dma((singles,)), dma, dma((singles,)), dma, dma,
        ],
        compiler_params=pltpu.CompilerParams(
            collective_id=0, has_side_effects=True, vmem_limit_bytes=VMEM_LIMIT
        ),
        name="fused_step",
    )(pair_lengths, labels, hidden.reshape(pairs, seq, width), attn_weight, norm_gain, pos_bias, score_weight)
    update, loss = pl.pallas_call(
        functools.partial(finish_kernel, duos),
        in_specs=[here, here],
        out_specs=[here, small],
        out_shape=[
            jax.ShapeDtypeStruct((rows, 4 * width), F32),
            jax.ShapeDtypeStruct((queries,), F32),
        ],
        name="finish",
    )(fin, loss)
    return (update, loss)


def solution(mesh):
    in_specs = (
        P("dp", "cand", None, None),
        P("dp", None),
        P(),
        P(),
        P(),
        P("dp", "cand"),
        P("dp", "cand"),
    )
    out_specs = (P("dp", None), P("dp"))
    return jax.shard_map(shards, mesh=mesh, in_specs=in_specs, out_specs=out_specs, check_vma=False)
```

```python
import functools

import jax
import jax.numpy as jnp
from jax import lax
from jax.experimental import pallas as pl
from jax.experimental.pallas import tpu as pltpu
from jax.sharding import PartitionSpec as P

EPS = 1e-06
F32 = jnp.float32
BF16 = jnp.bfloat16
VMEM_LIMIT = 60 * 1024 * 1024
LEAD = 4
FINISH = 2
NT = (((1,), (1,)), ((), ()))
TN = (((0,), (0,)), ((), ()))
MESH = pl.DeviceIdType.MESH


def half_masks(lanes):
    lane = lax.broadcasted_iota(jnp.int32, (1, lanes), 1)
    low = (lane < lanes // 2).astype(F32)
    return low.astype(BF16), (1.0 - low).astype(BF16)


def stack_halves(block, low, high):
    return jnp.concatenate([block * low, block * high], axis=0)


def head_mask(hpad, width, head_size):
    lane = lax.broadcasted_iota(jnp.int32, (hpad, width), 1)
    head = lax.broadcasted_iota(jnp.int32, (hpad, width), 0)
    start = head * head_size
    return ((lane >= start) & (lane < start + head_size)).astype(F32)


def arrived(ref, sem):
    pltpu.make_async_copy(ref, ref, sem).wait()


def push(src, dst, send, recv, target):
    pltpu.make_async_remote_copy(
        src_ref=src, dst_ref=dst, send_sem=send, recv_sem=recv, device_id=target, device_id_type=MESH
    ).start()


def lengths_column(ref, pairs, per):
    row = lax.broadcasted_iota(jnp.int32, (pairs, 1), 0)
    column = jnp.zeros((pairs, 1), F32)
    for i in range(pairs):
        column = jnp.where(row == i, ref[i // per, i % per].astype(F32), column)
    return column


def fused_kernel(n, m, early, len_hbm, lab_hbm, h_hbm, w_hbm, gain_hbm, bias_hbm, sw_hbm,
                 fin_hbm, loss_ref,
                 len_ref, lab_ref, gain_ref, sw_ref, small_sem, fin, h_scr, bias_scr, w_scr, norm_scr, nt_scr, qk_scr, p_scr, wsum_scr, u_scr, hsum_scr, ex_scr,
                 dp_scr, dqk_scr, grads, r1, s1, r2, s2, r3, s3, r4, a1, b1, a2, b2, a3, a4, sq, r6,
                 h_sem, b_sem, wa_sem, wb_sem,
                 za_r, xa_r, zb_r, xb_r, yb_r, ga_r, gb_r, few_s, many_s, ex_s, ex_r,
                 t1, v1, t2, v2, t3, v3, t4, v4, t5, v5, t6, v6,
                 e1, f1, e2, f2, e3, f3, e4, f4, e5, f5):
    pairs, seq, width = h_scr.shape
    queries, per = len_ref.shape
    heads = bias_scr.shape[0]
    groups, half, _, rows, lanes = w_scr.shape
    duos = heads // 2
    duo = m // 2
    head_size = width // heads
    hpad = u_scr.shape[1]
    batch = pairs // h_sem.shape[0]
    batches = pairs // batch
    early_rounds = early // 2
    late_rounds = (groups - early) // m
    d, c = lax.axis_index("dp"), lax.axis_index("cand")
    z, x = d // 2, d % 2
    y, core = c // 2, c % 2
    across = (d + 1 - 2 * x, c)
    other = (d, c + 1 - 2 * core)

    lead = LEAD

    def column(g):
        tail = g // (2 * duos)
        return (1 - tail) * (g // 2 + (g % 2) * duos) + tail * g

    peers = [(d, lax.rem(c + j, m)) for j in range(1, m)] + [(lax.rem(d + j, n), c) for j in range(1, n)]
    peers += [(lax.rem(d + j, n), other[1]) for j in range(1, n)]
    barrier = pltpu.get_barrier_semaphore()
    for peer in peers:
        pl.semaphore_signal(barrier, inc=1, device_id=peer, device_id_type=MESH)

    small = [(len_hbm, len_ref), (gain_hbm, gain_ref), (lab_hbm, lab_ref), (sw_hbm, sw_ref)]
    small = [pltpu.make_async_copy(src, dst, small_sem.at[t]) for t, (src, dst) in enumerate(small)]

    early_slots = (0, duos, groups - 4, groups - 2)

    def early_group(a, which):
        return early_slots[a] + which

    def late_group(r, which):
        if r == 0:
            return 2 + which + 2 * (which // 4)
        return 4 + r * m + which

    order = [("late", 0), ("early", 0), ("late", 1), ("early", 1), ("late", 2), ("early", 2), ("late", 3), ("early", 3)]
    order = [(kind, r) for kind, r in order if kind == "early" or r < late_rounds]

    def load(g, sem):
        at = pl.multiple_of(column(g) * lanes, lanes)
        return pltpu.make_async_copy(w_hbm.at[:, pl.ds(at, lanes)], w_scr.at[g, z, x], sem)

    loads = [load(early_group(a, core), wa_sem.at[a]) for a in range(early_rounds)]
    loads += [load(late_group(r, c), wb_sem.at[r, 0]) for r in range(late_rounds)]
    mirrors = [
        [load(late_group(r, 2 * lax.rem(y - j + duo, duo) + core), wb_sem.at[r, j]) for j in range(1, duo)]
        for r in range(late_rounds)
    ]
    tokens = []
    for b in range(batches):
        part = pl.ds(b * batch, batch)
        tokens.append(pltpu.make_async_copy(h_hbm.at[part], h_scr.at[part], h_sem.at[b]))
    bias_load = pltpu.make_async_copy(bias_hbm, bias_scr, b_sem)
    for copy in loads + small + tokens + [bias_load] + sum(mirrors, []):
        copy.start()
    col = lax.broadcasted_iota(jnp.int32, (1, seq), 1)
    row = lax.broadcasted_iota(jnp.int32, (seq, 1), 0)
    key = lax.broadcasted_iota(jnp.int32, (2, seq, seq), 1)
    low, high = half_masks(lanes)

    def length_of(i):
        return len_ref[i // per, i % per]

    def normalise(b):
        tokens[b].wait()
        values = h_scr[b * batch : (b + 1) * batch].reshape(batch * seq, width).astype(F32)
        factor = lax.rsqrt(jnp.mean(values * values, axis=-1, keepdims=True) + EPS)
        normed = (values * factor * gain).astype(BF16)
        norm_scr[b * batch : (b + 1) * batch] = normed.reshape(batch, seq, width)
        nt_scr[:, b * batch * seq : (b + 1) * batch * seq] = normed.T
        for j in range(batch):
            i = b * batch + j
            live = (row < length_of(i)).astype(F32)
            hsum_scr[i : i + 1, :] = jnp.sum(values[j * seq : (j + 1) * seq] * live, axis=0, keepdims=True)

    hops = [1] + [half - 1] * (half > 2) + list(range(2, half - 1))

    def send_z(g, s, r, x_s, x_r):
        block = w_scr.at[g, z, x]
        for j in hops:
            push(block, block, s, r.at[j - 1], (2 * lax.rem(z + j, half) + x, c))
        push(block, block, x_s, x_r, across)

    def relay_x(g, z_sem, s, r, also=None):
        for j in hops:
            block = w_scr.at[g, lax.rem(z - j + half, half), x]
            arrived(block, z_sem.at[j - 1])
            push(block, block, s, r, across)
            if also is not None:
                relay_y(block, also, 0)

    def send_round(i):
        if i >= len(order):
            return
        kind, r = order[i]
        if kind == "early":
            loads[r].wait()
            send_z(early_group(r, core), few_s, za_r.at[r], many_s, xa_r.at[r])
        else:
            loads[early_rounds + r].wait()
            send_z(late_group(r, c), few_s, zb_r.at[r], many_s, xb_r.at[r])

    def early_x(a):
        relay_x(early_group(a, core), za_r.at[a], many_s, xa_r.at[a])
        send_round(order.index(("early", a)) + lead)

    def early_core(a):
        g = early_group(a, core)
        arrived(w_scr.at[g, :, 0], xa_r.at[a])
        push(w_scr.at[g], w_scr.at[g], many_s, ga_r.at[a], other)

    def early_ready(a):
        g = early_group(a, 1 - core)
        arrived(w_scr.at[g], ga_r.at[a])

    def relay_y(blocks, r, place):
        for j in range(1, duo):
            target = (d, 2 * lax.rem(y + j, duo) + core)
            push(blocks, blocks, (few_s, many_s)[place], yb_r.at[r, place, j - 1], target)

    def late_x(r):
        relay_x(late_group(r, c), zb_r.at[r], many_s, xb_r.at[r], r)
        send_round(order.index(("late", r)) + lead)

    def late_y(r):
        g = late_group(r, c)
        arrived(w_scr.at[g, :, 0], xb_r.at[r])
        relay_y(w_scr.at[g, :, 1 - x], r, 1)
        push(w_scr.at[g], w_scr.at[g], many_s, gb_r.at[r], other)

    def late_core(r):
        for j in range(1, duo):
            g = late_group(r, 2 * lax.rem(y - j + duo, duo) + core)
            mirrors[r][j - 1].wait()
            arrived(w_scr.at[g, 0 : half - 1, 0], yb_r.at[r, 0, j - 1])
            arrived(w_scr.at[g, :, 0], yb_r.at[r, 1, j - 1])
            push(w_scr.at[g], w_scr.at[g], many_s, gb_r.at[r], other)

    def late_ready(r):
        arrived(w_scr.at[0:duo], gb_r.at[r])

    def relays(todo):
        for act, r in todo:
            if r < (early_rounds if act in (early_x, early_core, early_ready) else late_rounds):
                with jax.named_scope(act.__name__ + '_%d' % r):
                    act(r)

    with jax.named_scope('barrier'):
        pl.semaphore_wait(barrier, len(peers))
    for i in range(lead):
        send_round(i)
    for copy in small:
        copy.wait()
    gain = gain_ref[...].reshape(1, width)
    sw = sw_ref[...].reshape(1, width)
    with jax.named_scope('norm'):
        for b in range(batches):
            normalise(b)
    with jax.named_scope('bias'):
        bias_load.wait()
        for h in range(heads):
            bias_scr[h] = bias_scr[h].T
    with jax.named_scope('early'):
        relays([(late_x, 0), (early_x, 0), (late_y, 0), (late_x, 1), (early_core, 0), (early_ready, 0)])

    def weight(g):
        value = w_scr[g]
        if rows % 16 == 0:
            return value.reshape(width, lanes)
        return value.astype(F32).reshape(width, lanes).astype(BF16)

    def project(hp):
        both = jnp.concatenate([weight(2 * hp), weight(2 * hp + 1)], axis=1)
        for b in range(batches):
            block = norm_scr[b * batch : (b + 1) * batch].reshape(batch * seq, width)
            proj = jnp.dot(block, both, preferred_element_type=F32)
            qk_scr[hp, b * batch : (b + 1) * batch] = proj.astype(BF16).reshape(batch, seq, 2 * lanes)

    def attend(hp, i):
        length = length_of(i)
        live = (col < length).astype(F32)
        q2 = qk_scr[hp, i, :, :lanes]
        k2 = qk_scr[hp, i, :, lanes:]
        logits = lax.dot_general(stack_halves(k2, low, high), q2, NT, preferred_element_type=F32)
        logits = logits.reshape(2, seq, seq) + bias_scr[pl.ds(2 * hp, 2)]
        logits = jnp.where(key < length, logits, -1e30)
        expo = jnp.exp(logits - jnp.max(logits, axis=1, keepdims=True))
        inv = live[None] / jnp.sum(expo, axis=1, keepdims=True)
        probs = (expo * inv).astype(BF16)
        probs = jnp.stack([probs[0].T, probs[1].T])
        p_scr[hp, i] = probs
        wsum_scr[hp, i] = jnp.sum(probs.astype(F32), axis=1)

    forward_plan = {
        (0, 1): [(early_x, 1), (late_core, 0), (late_y, 1), (late_x, 2)],
        (1, 0): [(late_ready, 0)],
        (1, 1): [(early_core, 1), (early_x, 2)],
        (2, 1): [(late_y, 2), (late_core, 1), (late_x, 3)],
        (3, 0): [(early_ready, 1)],
        (3, 1): [(early_core, 2), (early_x, 3)],
        (4, 0): [(late_ready, 1), (late_y, 3)],
        (4, 1): [(late_core, 2)],
        (5, 0): [(early_core, 3)],
    }

    def forward_step(hp, carry):
        for place in range(2):
            with jax.named_scope('fw_relay'):
                for step in range(duos):
                    todo = forward_plan.get((step, place))
                    if todo:
                        @pl.when(hp == step)
                        def _():
                            relays(todo)

            @pl.when(hp < duos)
            def _():
                with jax.named_scope('fw_block'):
                    if place == 0:
                        project(hp)
                    else:
                        for i in range(pairs):
                            attend(hp, i)

        return carry

    lax.fori_loop(0, duos, forward_step, 0)
    with jax.named_scope('late_core'):
        relays([(late_core, 3)])
    with jax.named_scope('u'):
      for i in range(pairs):
        parts = [wsum_scr[j, i] for j in range(duos)]
        if hpad > heads:
            parts.append(jnp.zeros((hpad - heads, seq), F32))
        weights = jnp.concatenate(parts, axis=0).astype(BF16)
        u_scr[i] = jnp.dot(weights, norm_scr[i], preferred_element_type=F32).astype(BF16)
    with jax.named_scope('late_ready'):
      relays([(late_ready, 2), (late_ready, 3), (early_ready, 2), (early_ready, 3)])

    w_v = jnp.concatenate([weight(2 * duos + j) for j in range(duos)], axis=1)
    w_o = jnp.concatenate([weight(3 * duos + j) for j in range(duos)], axis=1)
    u = u_scr[...].reshape(pairs * hpad, width)
    mixed = jnp.dot(u, w_v, preferred_element_type=F32)
    mask = head_mask(hpad, width, head_size)
    ctx32 = jnp.sum(mixed.reshape(pairs, hpad, width) * mask[None], axis=1)
    ctx = ctx32.astype(BF16)
    share = 1.0 / lengths_column(len_ref, pairs, per)
    mean = ctx32 * share
    mean_high = mean.astype(BF16)
    mean_low = (mean - mean_high.astype(F32)).astype(BF16)
    both = jnp.dot(jnp.concatenate([mean_high, mean_low], axis=0), w_o, preferred_element_type=F32)
    pooled = hsum_scr[...] * share + both[:pairs] + both[pairs:]
    factor = lax.rsqrt(jnp.mean(pooled * pooled, axis=-1, keepdims=True) + EPS)
    score = jnp.sum(pooled * factor * sw, axis=-1, keepdims=True)
    label = lengths_column(lab_ref, pairs, per)
    score = jnp.broadcast_to(score, (pairs, lanes))
    label = jnp.broadcast_to(label, (pairs, lanes))
    ex_scr[c] = jnp.concatenate([score, label], axis=0)
    for j in range(1, m):
        push(ex_scr.at[c], ex_scr.at[c], ex_s, ex_r, (d, lax.rem(c + j, m)))

    dot = jnp.sum(pooled * sw, axis=-1, keepdims=True) * (1.0 / width)
    slope = (factor * sw - pooled * (factor * factor * factor * dot)) * share
    cg = lax.dot_general(slope.astype(BF16), w_o, NT, preferred_element_type=F32)
    spread = (cg[:, None, :] * mask[None]).astype(BF16).reshape(pairs * hpad, width)
    wc = lax.dot_general(spread, w_v, NT, preferred_element_type=F32)
    u_scr_wc = wc.astype(BF16).reshape(pairs, hpad, width)
    for i in range(pairs):
        part = jnp.dot(u_scr_wc[i], nt_scr[:, i * seq : (i + 1) * seq], preferred_element_type=F32)
        for j in range(duos):
            dp_scr[j, i] = part[2 * j : 2 * j + 2]

    with jax.named_scope('ex_wait'):
      arrived(ex_scr.at[0 : m - 1], ex_r)
    all_scores, all_labels = ex_scr[:, :pairs], ex_scr[:, pairs:]
    target = jnp.exp(all_labels)
    own_target = jnp.exp(label)
    query = lax.broadcasted_iota(jnp.int32, (pairs, lanes), 0) // per
    loss_row = lax.broadcasted_iota(jnp.int32, loss_ref.shape, 0)
    loss = jnp.zeros(loss_ref.shape, F32)
    score_grad = jnp.zeros((pairs, lanes), F32)

    def total(values):
        return jnp.sum(jnp.sum(values, axis=0), axis=0, keepdims=True)

    for q in range(queries):
        inside = (query == q)[None]
        highest = jnp.max(jnp.max(jnp.where(inside, all_scores, -3e38), axis=0), axis=0, keepdims=True)
        expsum = total(jnp.where(inside, jnp.exp(all_scores - highest[None]), 0.0))
        target_sum = total(jnp.where(inside, target, 0.0))
        target_dot = total(jnp.where(inside, target * all_scores, 0.0))
        loss = jnp.where(loss_row == q + 1, highest + jnp.log(expsum) - target_dot / target_sum, loss)
        own = jnp.exp(score - highest) / expsum - own_target / target_sum
        score_grad = jnp.where(query == q, own, score_grad)
    loss_ref[...] = loss
    sg = score_grad[:, :1]
    out_grad = (slope * sg).astype(BF16)
    spread = (cg * sg).astype(BF16).astype(F32)
    spread = (spread[:, None, :] * mask[None]).astype(BF16).reshape(pairs * hpad, width)
    gv = lax.dot_general(u, spread, TN, preferred_element_type=F32).astype(BF16)
    go = lax.dot_general(ctx, out_grad, TN, preferred_element_type=F32).astype(BF16)
    for t in range(2 * duos):
        source = (gv, go)[t // duos]
        at = (t % duos) * lanes
        grads[t // 2, t % 2] = source[:, at : at + lanes].reshape(half, 2, rows, lanes)
    for i in range(pairs):
        for j in range(duos):
            dp_scr[j, i] = dp_scr[j, i] * sg[i : i + 1]

    chunks = r1.shape[0]

    def finish_chunks(part, waiting, square):
        with jax.named_scope('chunk_wait'):
            if waiting:
                arrived(fin.at[0 : len(waiting) * (m - 1)], v5)
            for g in range(len(waiting) * m):
                part = part + square(2 * duos + g)
        return part

    def stage_core(k):
        push(grads.at[k * duo : (k + 1) * duo, 1 - core], r1.at[k], t1, v1.at[k], other)

    def stage_y(k):
        arrived(r1.at[k], v1.at[k])
        s1[k] = (grads[k * duo : (k + 1) * duo, core].astype(F32) + r1[k].astype(F32)).astype(BF16)
        for j in range(1, duo):
            peer = lax.rem(y + j, duo)
            push(s1.at[k, peer], r2.at[k, j - 1], t2, v2.at[k], (d, 2 * peer + core))

    def stage_x(k):
        value = s1[k, y].astype(F32)
        if duo > 1:
            arrived(r2.at[k], v2.at[k])
        for j in range(1, duo):
            value = value + r2[k, j - 1].astype(F32)
        s2[k] = value.astype(BF16)
        push(s2.at[k, :, 1 - x], r3.at[k], t3, v3.at[k], across)

    def stage_z(k):
        arrived(r3.at[k], v3.at[k])
        s3[k] = (s2[k, :, x].astype(F32) + r3[k].astype(F32)).astype(BF16)
        for j in range(1, half):
            peer = lax.rem(z + j, half)
            push(s3.at[k, peer], r4.at[k, j - 1], t4, v4.at[k], (2 * peer + x, c))

    def stage_cand(k):
        value = s3[k, z].astype(F32)
        if half > 1:
            arrived(r4.at[k], v4.at[k])
        for j in range(1, half):
            value = value + r4[k, j - 1].astype(F32)
        piece = fin.at[2 * duos + k * m + c]
        piece[...] = value.astype(BF16)
        for j in range(1, m):
            push(piece, piece, t5, v5, (d, lax.rem(c + j, m)))

    def pair_column(k, which):
        at = chunks * duo + k
        if at < duos:
            return 2 * duos + 2 * at + which
        return at - duos + which * duos

    def pair_core(k):
        push(grads.at[chunks * duo + k, 1 - core], a1.at[k], e1, f1.at[k], other)

    def pair_x(k):
        arrived(a1.at[k], f1.at[k])
        b1[k] = (grads[chunks * duo + k, core].astype(F32) + a1[k].astype(F32)).astype(BF16)
        push(b1.at[k, :, 1 - x], a2.at[k], e2, f2.at[k], across)

    def pair_z(k):
        arrived(a2.at[k], f2.at[k])
        b2[k] = (b1[k, :, x].astype(F32) + a2[k].astype(F32)).astype(BF16)
        for j in range(1, half):
            peer = lax.rem(z + j, half)
            push(b2.at[k, peer], a3.at[k, j - 1], e3, f3.at[k], (2 * peer + x, c))

    def pair_y(k):
        value = b2[k, z].astype(F32)
        if half > 1:
            arrived(a3.at[k], f3.at[k])
        for j in range(1, half):
            value = value + a3[k, j - 1].astype(F32)
        a4[k, y] = value.astype(BF16)
        for j in range(1, duo):
            target = (d, 2 * lax.rem(y + j, duo) + core)
            push(a4.at[k, y], a4.at[k, y], e4, f4.at[k], target)

    def pair_done(k):
        if duo > 1:
            arrived(a4.at[k, 0 : duo - 1], f4.at[k])
        value = a4[k, 0].astype(F32)
        for j in range(1, duo):
            value = value + a4[k, j].astype(F32)
        piece = fin.at[pair_column(k, core)]
        piece[...] = value.astype(BF16)
        push(piece, piece, e5, f5, other)

    stages = (stage_core, stage_y, stage_x, stage_z, stage_cand)
    pair_stages = (pair_core, pair_x, pair_z, pair_y, pair_done)
    singles = a1.shape[0]
    step_time = 2.25
    plan = []
    for k in range(chunks):
        for stage, at in enumerate((0.0, 1.3 + 0.5 * k, 7.7 + 4.2 * k, 12.4 + 4.2 * k, 18.0 + 4.2 * k)):
            plan.append((at, stage, stages[stage], k))
    for k in range(singles):
        hp = chunks * duo + k - duos
        ready = step_time * (hp + 1) - 0.05 if hp >= 0 else 0.0
        for stage, at in enumerate((0.0, 1.2, 5.6, 11.0, 14.0)):
            plan.append((ready + at, 5 + stage, pair_stages[stage], k))
    plan.sort(key=lambda item: (item[0], item[1] % 5, item[3]))
    slots = [(step_time * hp + at, hp, place) for hp in range(duos)
             for place, at in enumerate((0.0, 1.3, step_time - 0.05))]
    homes = {}
    for item in plan:
        home = next(((hp, place) for at, hp, place in slots if at >= item[0] - 0.1), None)
        homes.setdefault(home, []).append(item)

    def run(hp, place):
        with jax.named_scope('bw_run'):
            for step in range(duos):
                items = homes.get((step, place))
                if items:
                    @pl.when(hp == step)
                    def _():
                        for _, stage, act, k in items:
                            with jax.named_scope('in_%d_%d' % (stage, k)):
                                act(k)

    def differentiate(hp, i):
        probs = p_scr[hp, i].astype(F32)
        term = probs * dp_scr[hp, i][:, None, :]
        dlog = (term - probs * jnp.sum(term, axis=-1, keepdims=True)).astype(BF16)
        wide = jnp.concatenate([dlog[0], dlog[1]], axis=1)
        q2 = stack_halves(qk_scr[hp, i, :, :lanes], low, high)
        k2 = stack_halves(qk_scr[hp, i, :, lanes:], low, high)
        dq = jnp.dot(wide, k2, preferred_element_type=F32)
        dk = lax.dot_general(dlog.reshape(2 * seq, seq), q2, TN, preferred_element_type=F32)
        dqk_scr[i, :, :lanes] = dq.astype(BF16)
        dqk_scr[i, :, lanes:] = dk.astype(BF16)

    def backward_step(hp, carry):
        run(hp, 0)

        @pl.when(hp < duos)
        def _():
            with jax.named_scope('bw_block'):
                for i in range(pairs):
                    differentiate(hp, i)

        run(hp, 1)

        @pl.when(hp < duos)
        def _():
            with jax.named_scope('bw_dot'):
                grad = jnp.dot(nt_scr[...], dqk_scr[...].reshape(pairs * seq, 2 * lanes), preferred_element_type=F32)
                grads[duos + hp, 0] = grad[:, :lanes].reshape(half, 2, rows, lanes).astype(BF16)
                grads[duos + hp, 1] = grad[:, lanes:].reshape(half, 2, rows, lanes).astype(BF16)

        run(hp, 2)
        return carry

    lax.fori_loop(0, duos, backward_step, 0)
    def square(g):
        block = fin[g].astype(F32).reshape(rows // 8, 8, lanes)
        return jnp.sum(block * block, axis=0)

    part = jnp.zeros((8, lanes), F32)
    waiting = [k for k in range(chunks)]
    for _, stage, act, k in homes.get(None, []):
        if stage == 9 and waiting and k == singles - 1:
            part = finish_chunks(part, waiting, square)
            waiting = []
        with jax.named_scope('tail_%d_%d' % (stage, k)):
            act(k)
    if waiting:
        part = finish_chunks(part, waiting, square)
    part = jnp.where(core == 0, part, 0.0)
    for k in range(singles):
        part = part + square(pair_column(k, core))
    sq[...] = part
    mine = core * n + d
    r6[mine] = part
    targets = [(lax.rem(d + j, n), core) for j in range(1, n)] + [(lax.rem(d + j, n), 1 - core) for j in range(n)]
    for t, (to, to_core) in enumerate(targets):
        push(sq, r6.at[mine], t6, v6, (to, c - core + to_core))
    with jax.named_scope('fin_wait'):
        arrived(fin.at[0:singles], f5)
    store = pltpu.make_async_copy(fin, fin_hbm, b_sem)
    store.start()
    with jax.named_scope('drain'):
        kinds = early_rounds + late_rounds * duo
        arrived(w_scr.at[0:kinds, 0 : half - 1, 0], few_s)
        arrived(w_scr.at[0 : 3 * kinds // 2], many_s)
        arrived(ex_scr.at[0 : m - 1], ex_s)
        if chunks:
            arrived(r1, t1)
            arrived(r3, t3)
            arrived(fin.at[0 : chunks * (m - 1)], t5)
            if duo > 1:
                arrived(r2, t2)
            if half > 1:
                arrived(r4, t4)
        arrived(a1, e1)
        arrived(a2, e2)
        arrived(fin.at[0:singles], e5)
        if half > 1:
            arrived(a3, e3)
        if duo > 1:
            arrived(a4.at[:, 0 : duo - 1], e4)
    with jax.named_scope('sq_wait'):
        arrived(r6.at[0 : 2 * n - 1], v6)
        arrived(r6.at[0 : 2 * n - 1], t6)
    count = groups * lanes * n * rows
    squares = jnp.sum(r6[...], axis=0)
    squares = jnp.sum(jnp.sum(squares, axis=0, keepdims=True), axis=1, keepdims=True)
    loss_ref[0:1, :] = jnp.broadcast_to(1.0 / (jnp.sqrt(squares / count) + EPS), (1, lanes))
    store.wait()


def finish_kernel(fin, loss_in, out_ref, loss_ref):
    columns, _, lanes = fin.shape
    scale = loss_in[0:1, :]
    for at in range(columns):
        out_ref[:, at * lanes : (at + 1) * lanes] = fin[at].astype(F32) * scale
    for q in range(loss_ref.shape[0]):
        loss_ref[q] = jnp.max(loss_in[q + 1 : q + 2, :])


def shards(hidden, attn_weight, norm_gain, pos_bias, score_weight, pair_lengths, labels):
    queries, per, seq, width = hidden.shape
    pairs = queries * per
    heads = pos_bias.shape[0]
    n, m = lax.axis_size("dp"), lax.axis_size("cand")
    lanes = 2 * (width // heads)
    duos = heads // 2
    groups = 4 * duos
    rows, half, duo = width // n, n // 2, m // 2
    early = groups // 3
    early_rounds, late_rounds = early // 2, (groups - early) // m
    batch = 4 if pairs % 4 == 0 else 1
    hpad = -(-heads // 16) * 16
    chunks = max(duos // duo - 1, 1)
    singles = 2 * duos - chunks * duo
    near, far = max(duo - 1, 1), max(half - 1, 1)
    dma = pltpu.SemaphoreType.DMA
    vmem = pltpu.VMEM
    here = pl.BlockSpec(memory_space=pltpu.VMEM)
    away = pl.BlockSpec(memory_space=pl.ANY)
    small = pl.BlockSpec(memory_space=pltpu.SMEM)
    loss_rows = -(-(queries + 1) // 8) * 8
    fin, loss = pl.pallas_call(
        functools.partial(fused_kernel, n, m, early),
        in_specs=[away] * 7,
        out_specs=[away, here],
        out_shape=[
            jax.ShapeDtypeStruct((groups, rows, lanes), BF16),
            jax.ShapeDtypeStruct((loss_rows, lanes), F32),
        ],
        scratch_shapes=[
            pltpu.SMEM((queries, per), jnp.int32),
            pltpu.SMEM((queries, per), jnp.int32),
            vmem((width,), F32),
            vmem((width,), F32),
            dma((4,)),
            vmem((groups, rows, lanes), BF16),
            vmem((pairs, seq, width), BF16),
            vmem(pos_bias.shape, F32),
            vmem((groups, half, 2, rows, lanes), BF16),
            vmem((pairs, seq, width), BF16),
            vmem((width, pairs * seq), BF16),
            vmem((duos, pairs, seq, 2 * lanes), BF16),
            vmem((duos, pairs, 2, seq, seq), BF16),
            vmem((duos, pairs, 2, seq), F32),
            vmem((pairs, hpad, width), BF16),
            vmem((pairs, width), F32),
            vmem((m, 2 * pairs, lanes), F32),
            vmem((duos, pairs, 2, seq), F32),
            vmem((pairs, seq, 2 * lanes), BF16),
            vmem((2 * duos, 2, half, 2, rows, lanes), BF16),
            vmem((chunks, duo, half, 2, rows, lanes), BF16),
            vmem((chunks, duo, half, 2, rows, lanes), BF16),
            vmem((chunks, near, half, 2, rows, lanes), BF16),
            vmem((chunks, half, 2, rows, lanes), BF16),
            vmem((chunks, half, rows, lanes), BF16),
            vmem((chunks, half, rows, lanes), BF16),
            vmem((chunks, far, rows, lanes), BF16),
            vmem((singles, half, 2, rows, lanes), BF16),
            vmem((singles, half, 2, rows, lanes), BF16),
            vmem((singles, half, rows, lanes), BF16),
            vmem((singles, half, rows, lanes), BF16),
            vmem((singles, far, rows, lanes), BF16),
            vmem((singles, duo, rows, lanes), BF16),
            vmem((8, lanes), F32),
            vmem((2 * n, 8, lanes), F32),
            dma((pairs // batch,)), dma, dma((early_rounds,)), dma((late_rounds, duo)),
            dma((early_rounds, far)), dma((early_rounds,)), dma((late_rounds, far)), dma((late_rounds,)),
            dma((late_rounds, 2, near)), dma((early_rounds,)), dma((late_rounds,)), dma, dma, dma, dma,
            dma, dma((chunks,)), dma, dma((chunks,)), dma, dma((chunks,)), dma, dma((chunks,)), dma, dma, dma, dma,
            dma, dma((singles,)), dma, dma((singles,)), dma, dma((singles,)), dma, dma((singles,)), dma, dma,
        ],
        compiler_params=pltpu.CompilerParams(
            collective_id=0, has_side_effects=True, vmem_limit_bytes=VMEM_LIMIT
        ),
        name="fused_step",
    )(pair_lengths, labels, hidden.reshape(pairs, seq, width), attn_weight, norm_gain, pos_bias, score_weight)
    update, loss = pl.pallas_call(
        finish_kernel,
        grid=(FINISH,),
        in_specs=[
            pl.BlockSpec((groups // FINISH, rows, lanes), lambda i: (i, 0, 0)),
            pl.BlockSpec(loss.shape, lambda i: (0, 0)),
        ],
        out_specs=[pl.BlockSpec((rows, 4 * width // FINISH), lambda i: (0, i)), small],
        out_shape=[
            jax.ShapeDtypeStruct((rows, 4 * width), F32),
            jax.ShapeDtypeStruct((queries,), F32),
        ],
        name="finish",
    )(fin, loss)
    return (update, loss)


def solution(mesh):
    in_specs = (
        P("dp", "cand", None, None),
        P("dp", None),
        P(),
        P(),
        P(),
        P("dp", "cand"),
        P("dp", "cand"),
    )
    out_specs = (P("dp", None), P("dp"))
    return jax.shard_map(shards, mesh=mesh, in_specs=in_specs, out_specs=out_specs, check_vma=False)
```

```python
import functools

import jax
import jax.numpy as jnp
from jax import lax
from jax.experimental import pallas as pl
from jax.experimental.pallas import tpu as pltpu
from jax.sharding import PartitionSpec as P

EPS = 1e-06
F32 = jnp.float32
BF16 = jnp.bfloat16
VMEM_LIMIT = 60 * 1024 * 1024
LEAD = 4
FINISH = 2
NT = (((1,), (1,)), ((), ()))
TN = (((0,), (0,)), ((), ()))
MESH = pl.DeviceIdType.MESH


def half_masks(lanes):
    lane = lax.broadcasted_iota(jnp.int32, (1, lanes), 1)
    low = (lane < lanes // 2).astype(F32)
    return low.astype(BF16), (1.0 - low).astype(BF16)


def stack_halves(block, low, high):
    return jnp.concatenate([block * low, block * high], axis=0)


def head_mask(hpad, width, head_size):
    lane = lax.broadcasted_iota(jnp.int32, (hpad, width), 1)
    head = lax.broadcasted_iota(jnp.int32, (hpad, width), 0)
    start = head * head_size
    return ((lane >= start) & (lane < start + head_size)).astype(F32)


def arrived(ref, sem):
    pltpu.make_async_copy(ref, ref, sem).wait()


def push(src, dst, send, recv, target):
    pltpu.make_async_remote_copy(
        src_ref=src, dst_ref=dst, send_sem=send, recv_sem=recv, device_id=target, device_id_type=MESH
    ).start()


def lengths_column(ref, pairs, per):
    row = lax.broadcasted_iota(jnp.int32, (pairs, 1), 0)
    column = jnp.zeros((pairs, 1), F32)
    for i in range(pairs):
        column = jnp.where(row == i, ref[i // per, i % per].astype(F32), column)
    return column


def fused_kernel(n, m, early, len_hbm, lab_hbm, h_hbm, w_hbm, gain_hbm, bias_hbm, sw_hbm,
                 fin_hbm, loss_ref,
                 len_ref, lab_ref, gain_ref, sw_ref, small_sem, fin, h_scr, bias_scr, w_scr, norm_scr, nt_scr, qk_scr, p_scr, wsum_scr, u_scr, hsum_scr, ex_scr,
                 dp_scr, dqk_scr, grads, r1, s1, r2, s2, r3, s3, r4, a1, b1, a2, b2, a3, a4, sq, r6,
                 h_sem, b_sem, wa_sem, wb_sem,
                 za_r, xa_r, zb_r, xb_r, yb_r, ga_r, gb_r, few_s, many_s, ex_s, ex_r,
                 t1, v1, t2, v2, t3, v3, t4, v4, t5, v5, t6, v6,
                 e1, f1, e2, f2, e3, f3, e4, f4, e5, f5):
    pairs, seq, width = h_scr.shape
    queries, per = len_ref.shape
    heads = bias_scr.shape[0]
    groups, half, _, rows, lanes = w_scr.shape
    duos = heads // 2
    duo = m // 2
    head_size = width // heads
    hpad = u_scr.shape[1]
    batch = pairs // h_sem.shape[0]
    batches = pairs // batch
    early_rounds = early // 2
    late_rounds = (groups - early) // m
    d, c = lax.axis_index("dp"), lax.axis_index("cand")
    z, x = d // 2, d % 2
    y, core = c // 2, c % 2
    across = (d + 1 - 2 * x, c)
    other = (d, c + 1 - 2 * core)

    lead = LEAD

    def column(g):
        tail = g // (2 * duos)
        return (1 - tail) * (g // 2 + (g % 2) * duos) + tail * g

    peers = [(d, lax.rem(c + j, m)) for j in range(1, m)] + [(lax.rem(d + j, n), c) for j in range(1, n)]
    peers += [(lax.rem(d + j, n), other[1]) for j in range(1, n)]
    barrier = pltpu.get_barrier_semaphore()
    for peer in peers:
        pl.semaphore_signal(barrier, inc=1, device_id=peer, device_id_type=MESH)

    small = [(len_hbm, len_ref), (gain_hbm, gain_ref), (lab_hbm, lab_ref), (sw_hbm, sw_ref)]
    small = [pltpu.make_async_copy(src, dst, small_sem.at[t]) for t, (src, dst) in enumerate(small)]

    early_slots = (0, duos, groups - 4, groups - 2)

    def early_group(a, which):
        return early_slots[a] + which

    def late_group(r, which):
        if r == 0:
            return 2 + which + 2 * (which // 4)
        return 4 + r * m + which

    order = [("late", 0), ("early", 0), ("late", 1), ("early", 1), ("late", 2), ("early", 2), ("late", 3), ("early", 3)]
    order = [(kind, r) for kind, r in order if kind == "early" or r < late_rounds]

    def load(g, sem):
        at = pl.multiple_of(column(g) * lanes, lanes)
        return pltpu.make_async_copy(w_hbm.at[:, pl.ds(at, lanes)], w_scr.at[g, z, x], sem)

    loads = [load(early_group(a, core), wa_sem.at[a]) for a in range(early_rounds)]
    loads += [load(late_group(r, c), wb_sem.at[r, 0]) for r in range(late_rounds)]
    mirrors = [
        [load(late_group(r, 2 * lax.rem(y - j + duo, duo) + core), wb_sem.at[r, j]) for j in range(1, duo)]
        for r in range(late_rounds)
    ]
    tokens = []
    for b in range(batches):
        part = pl.ds(b * batch, batch)
        tokens.append(pltpu.make_async_copy(h_hbm.at[part], h_scr.at[part], h_sem.at[b]))
    bias_load = pltpu.make_async_copy(bias_hbm, bias_scr, b_sem)
    for copy in loads + small + tokens + [bias_load] + sum(mirrors, []):
        copy.start()
    col = lax.broadcasted_iota(jnp.int32, (1, seq), 1)
    row = lax.broadcasted_iota(jnp.int32, (seq, 1), 0)
    key = lax.broadcasted_iota(jnp.int32, (2, seq, seq), 1)
    low, high = half_masks(lanes)

    def length_of(i):
        return len_ref[i // per, i % per]

    def normalise(b):
        tokens[b].wait()
        values = h_scr[b * batch : (b + 1) * batch].reshape(batch * seq, width).astype(F32)
        factor = lax.rsqrt(jnp.mean(values * values, axis=-1, keepdims=True) + EPS)
        normed = (values * factor * gain).astype(BF16)
        norm_scr[b * batch : (b + 1) * batch] = normed.reshape(batch, seq, width)
        nt_scr[:, b * batch * seq : (b + 1) * batch * seq] = normed.T
        for j in range(batch):
            i = b * batch + j
            live = (row < length_of(i)).astype(F32)
            hsum_scr[i : i + 1, :] = jnp.sum(values[j * seq : (j + 1) * seq] * live, axis=0, keepdims=True)

    hops = [1] + [half - 1] * (half > 2) + list(range(2, half - 1))

    def send_z(g, s, r, x_s, x_r):
        block = w_scr.at[g, z, x]
        for j in hops:
            push(block, block, s, r.at[j - 1], (2 * lax.rem(z + j, half) + x, c))
        push(block, block, x_s, x_r, across)

    def relay_x(g, z_sem, s, r, also=None):
        for j in hops:
            block = w_scr.at[g, lax.rem(z - j + half, half), x]
            arrived(block, z_sem.at[j - 1])
            push(block, block, s, r, across)
            if also is not None:
                relay_y(block, also, 0)

    def send_round(i):
        if i >= len(order):
            return
        kind, r = order[i]
        if kind == "early":
            loads[r].wait()
            send_z(early_group(r, core), few_s, za_r.at[r], many_s, xa_r.at[r])
        else:
            loads[early_rounds + r].wait()
            send_z(late_group(r, c), few_s, zb_r.at[r], many_s, xb_r.at[r])

    def early_x(a):
        relay_x(early_group(a, core), za_r.at[a], many_s, xa_r.at[a])
        send_round(order.index(("early", a)) + lead)

    def early_core(a):
        g = early_group(a, core)
        arrived(w_scr.at[g, :, 0], xa_r.at[a])
        push(w_scr.at[g], w_scr.at[g], many_s, ga_r.at[a], other)

    def early_ready(a):
        g = early_group(a, 1 - core)
        arrived(w_scr.at[g], ga_r.at[a])

    def relay_y(blocks, r, place):
        for j in range(1, duo):
            target = (d, 2 * lax.rem(y + j, duo) + core)
            push(blocks, blocks, (few_s, many_s)[place], yb_r.at[r, place, j - 1], target)

    def late_x(r):
        relay_x(late_group(r, c), zb_r.at[r], many_s, xb_r.at[r], r)
        send_round(order.index(("late", r)) + lead)

    def late_y(r):
        g = late_group(r, c)
        arrived(w_scr.at[g, :, 0], xb_r.at[r])
        relay_y(w_scr.at[g, :, 1 - x], r, 1)
        push(w_scr.at[g], w_scr.at[g], many_s, gb_r.at[r], other)

    def late_core(r):
        for j in range(1, duo):
            g = late_group(r, 2 * lax.rem(y - j + duo, duo) + core)
            mirrors[r][j - 1].wait()
            arrived(w_scr.at[g, 0 : half - 1, 0], yb_r.at[r, 0, j - 1])
            arrived(w_scr.at[g, :, 0], yb_r.at[r, 1, j - 1])
            push(w_scr.at[g], w_scr.at[g], many_s, gb_r.at[r], other)

    def late_ready(r):
        arrived(w_scr.at[0:duo], gb_r.at[r])

    def relays(todo):
        for act, r in todo:
            if r < (early_rounds if act in (early_x, early_core, early_ready) else late_rounds):
                with jax.named_scope(act.__name__ + '_%d' % r):
                    act(r)

    with jax.named_scope('barrier'):
        pl.semaphore_wait(barrier, len(peers))
    for i in range(lead):
        send_round(i)
    for copy in small:
        copy.wait()
    gain = gain_ref[...].reshape(1, width)
    sw = sw_ref[...].reshape(1, width)
    with jax.named_scope('norm'):
        for b in range(batches):
            normalise(b)
    with jax.named_scope('bias'):
        bias_load.wait()
        for h in range(heads):
            bias_scr[h] = bias_scr[h].T
    with jax.named_scope('early'):
        relays([(late_x, 0), (early_x, 0), (late_y, 0), (late_x, 1), (early_core, 0), (early_ready, 0)])

    def weight(g):
        value = w_scr[g]
        if rows % 16 == 0:
            return value.reshape(width, lanes)
        return value.astype(F32).reshape(width, lanes).astype(BF16)

    def project(hp):
        both = jnp.concatenate([weight(2 * hp), weight(2 * hp + 1)], axis=1)
        for b in range(batches):
            block = norm_scr[b * batch : (b + 1) * batch].reshape(batch * seq, width)
            proj = jnp.dot(block, both, preferred_element_type=F32)
            qk_scr[hp, b * batch : (b + 1) * batch] = proj.astype(BF16).reshape(batch, seq, 2 * lanes)

    def attend(hp, i):
        length = length_of(i)
        live = (col < length).astype(F32)
        q2 = qk_scr[hp, i, :, :lanes]
        k2 = qk_scr[hp, i, :, lanes:]
        logits = lax.dot_general(stack_halves(k2, low, high), q2, NT, preferred_element_type=F32)
        logits = logits.reshape(2, seq, seq) + bias_scr[pl.ds(2 * hp, 2)]
        logits = jnp.where(key < length, logits, -1e30)
        expo = jnp.exp(logits - jnp.max(logits, axis=1, keepdims=True))
        inv = live[None] / jnp.sum(expo, axis=1, keepdims=True)
        probs = (expo * inv).astype(BF16)
        probs = jnp.stack([probs[0].T, probs[1].T])
        p_scr[hp, i] = probs
        wsum_scr[hp, i] = jnp.sum(probs.astype(F32), axis=1)

    forward_plan = {
        (0, 1): [(early_x, 1), (late_core, 0), (late_y, 1), (late_x, 2)],
        (1, 0): [(late_ready, 0)],
        (1, 1): [(early_core, 1), (early_x, 2)],
        (2, 1): [(late_y, 2), (late_core, 1), (late_x, 3)],
        (3, 0): [(early_ready, 1)],
        (3, 1): [(early_core, 2), (early_x, 3)],
        (4, 0): [(late_ready, 1), (late_y, 3)],
        (4, 1): [(late_core, 2)],
        (5, 0): [(early_core, 3)],
    }

    def forward_step(hp, carry):
        for place in range(2):
            with jax.named_scope('fw_relay'):
                for step in range(duos):
                    todo = forward_plan.get((step, place))
                    if todo:
                        @pl.when(hp == step)
                        def _():
                            relays(todo)

            @pl.when(hp < duos)
            def _():
                with jax.named_scope('fw_block'):
                    if place == 0:
                        project(hp)
                    else:
                        for i in range(pairs):
                            attend(hp, i)

        return carry

    lax.fori_loop(0, duos, forward_step, 0)
    with jax.named_scope('late_core'):
        relays([(late_core, 3)])
    with jax.named_scope('u'):
      for i in range(pairs):
        parts = [wsum_scr[j, i] for j in range(duos)]
        if hpad > heads:
            parts.append(jnp.zeros((hpad - heads, seq), F32))
        weights = jnp.concatenate(parts, axis=0).astype(BF16)
        u_scr[i] = jnp.dot(weights, norm_scr[i], preferred_element_type=F32).astype(BF16)
    with jax.named_scope('late_ready'):
      relays([(late_ready, 2), (late_ready, 3), (early_ready, 2), (early_ready, 3)])

    w_v = jnp.concatenate([weight(2 * duos + j) for j in range(duos)], axis=1)
    w_o = jnp.concatenate([weight(3 * duos + j) for j in range(duos)], axis=1)
    u = u_scr[...].reshape(pairs * hpad, width)
    mixed = jnp.dot(u, w_v, preferred_element_type=F32)
    mask = head_mask(hpad, width, head_size)
    ctx32 = jnp.sum(mixed.reshape(pairs, hpad, width) * mask[None], axis=1)
    ctx = ctx32.astype(BF16)
    share = 1.0 / lengths_column(len_ref, pairs, per)
    mean = ctx32 * share
    mean_high = mean.astype(BF16)
    mean_low = (mean - mean_high.astype(F32)).astype(BF16)
    both = jnp.dot(jnp.concatenate([mean_high, mean_low], axis=0), w_o, preferred_element_type=F32)
    pooled = hsum_scr[...] * share + both[:pairs] + both[pairs:]
    factor = lax.rsqrt(jnp.mean(pooled * pooled, axis=-1, keepdims=True) + EPS)
    score = jnp.sum(pooled * factor * sw, axis=-1, keepdims=True)
    label = lengths_column(lab_ref, pairs, per)
    score = jnp.broadcast_to(score, (pairs, lanes))
    label = jnp.broadcast_to(label, (pairs, lanes))
    ex_scr[c] = jnp.concatenate([score, label], axis=0)
    for j in range(1, m):
        push(ex_scr.at[c], ex_scr.at[c], ex_s, ex_r, (d, lax.rem(c + j, m)))

    dot = jnp.sum(pooled * sw, axis=-1, keepdims=True) * (1.0 / width)
    slope = (factor * sw - pooled * (factor * factor * factor * dot)) * share
    cg = lax.dot_general(slope.astype(BF16), w_o, NT, preferred_element_type=F32)
    spread = (cg[:, None, :] * mask[None]).astype(BF16).reshape(pairs * hpad, width)
    wc = lax.dot_general(spread, w_v, NT, preferred_element_type=F32)
    u_scr_wc = wc.astype(BF16).reshape(pairs, hpad, width)
    for i in range(pairs):
        part = jnp.dot(u_scr_wc[i], nt_scr[:, i * seq : (i + 1) * seq], preferred_element_type=F32)
        for j in range(duos):
            dp_scr[j, i] = part[2 * j : 2 * j + 2]

    with jax.named_scope('ex_wait'):
      arrived(ex_scr.at[0 : m - 1], ex_r)
    all_scores, all_labels = ex_scr[:, :pairs], ex_scr[:, pairs:]
    target = jnp.exp(all_labels)
    own_target = jnp.exp(label)
    query = lax.broadcasted_iota(jnp.int32, (pairs, lanes), 0) // per
    loss_row = lax.broadcasted_iota(jnp.int32, loss_ref.shape, 0)
    loss = jnp.zeros(loss_ref.shape, F32)
    score_grad = jnp.zeros((pairs, lanes), F32)

    def total(values):
        return jnp.sum(jnp.sum(values, axis=0), axis=0, keepdims=True)

    for q in range(queries):
        inside = (query == q)[None]
        highest = jnp.max(jnp.max(jnp.where(inside, all_scores, -3e38), axis=0), axis=0, keepdims=True)
        expsum = total(jnp.where(inside, jnp.exp(all_scores - highest[None]), 0.0))
        target_sum = total(jnp.where(inside, target, 0.0))
        target_dot = total(jnp.where(inside, target * all_scores, 0.0))
        loss = jnp.where(loss_row == q + 1, highest + jnp.log(expsum) - target_dot / target_sum, loss)
        own = jnp.exp(score - highest) / expsum - own_target / target_sum
        score_grad = jnp.where(query == q, own, score_grad)
    loss_ref[...] = loss
    sg = score_grad[:, :1]
    out_grad = (slope * sg).astype(BF16)
    spread = (cg * sg).astype(BF16).astype(F32)
    spread = (spread[:, None, :] * mask[None]).astype(BF16).reshape(pairs * hpad, width)
    chunks = r1.shape[0]

    def finish_chunks(part, waiting, square):
        with jax.named_scope('chunk_wait'):
            if waiting:
                arrived(fin.at[0 : len(waiting) * (m - 1)], v5)
            for g in range(len(waiting) * m):
                part = part + square(2 * duos + g)
        return part

    def stage_core(k):
        push(grads.at[k * duo : (k + 1) * duo, 1 - core], r1.at[k], t1, v1.at[k], other)

    def stage_y(k):
        arrived(r1.at[k], v1.at[k])
        s1[k] = (grads[k * duo : (k + 1) * duo, core].astype(F32) + r1[k].astype(F32)).astype(BF16)
        for j in range(1, duo):
            peer = lax.rem(y + j, duo)
            push(s1.at[k, peer], r2.at[k, j - 1], t2, v2.at[k], (d, 2 * peer + core))

    def stage_x(k):
        value = s1[k, y].astype(F32)
        if duo > 1:
            arrived(r2.at[k], v2.at[k])
        for j in range(1, duo):
            value = value + r2[k, j - 1].astype(F32)
        s2[k] = value.astype(BF16)
        push(s2.at[k, :, 1 - x], r3.at[k], t3, v3.at[k], across)

    def stage_z(k):
        arrived(r3.at[k], v3.at[k])
        s3[k] = (s2[k, :, x].astype(F32) + r3[k].astype(F32)).astype(BF16)
        for j in range(1, half):
            peer = lax.rem(z + j, half)
            push(s3.at[k, peer], r4.at[k, j - 1], t4, v4.at[k], (2 * peer + x, c))

    def stage_cand(k):
        value = s3[k, z].astype(F32)
        if half > 1:
            arrived(r4.at[k], v4.at[k])
        for j in range(1, half):
            value = value + r4[k, j - 1].astype(F32)
        piece = fin.at[2 * duos + k * m + c]
        piece[...] = value.astype(BF16)
        for j in range(1, m):
            push(piece, piece, t5, v5, (d, lax.rem(c + j, m)))

    def pair_column(k, which):
        at = chunks * duo + k
        if at < duos:
            return 2 * duos + 2 * at + which
        return at - duos + which * duos

    def pair_core(k):
        push(grads.at[chunks * duo + k, 1 - core], a1.at[k], e1, f1.at[k], other)

    def pair_x(k):
        arrived(a1.at[k], f1.at[k])
        b1[k] = (grads[chunks * duo + k, core].astype(F32) + a1[k].astype(F32)).astype(BF16)
        push(b1.at[k, :, 1 - x], a2.at[k], e2, f2.at[k], across)

    def pair_z(k):
        arrived(a2.at[k], f2.at[k])
        b2[k] = (b1[k, :, x].astype(F32) + a2[k].astype(F32)).astype(BF16)
        for j in range(1, half):
            peer = lax.rem(z + j, half)
            push(b2.at[k, peer], a3.at[k, j - 1], e3, f3.at[k], (2 * peer + x, c))

    def pair_y(k):
        value = b2[k, z].astype(F32)
        if half > 1:
            arrived(a3.at[k], f3.at[k])
        for j in range(1, half):
            value = value + a3[k, j - 1].astype(F32)
        a4[k, y] = value.astype(BF16)
        for j in range(1, duo):
            target = (d, 2 * lax.rem(y + j, duo) + core)
            push(a4.at[k, y], a4.at[k, y], e4, f4.at[k], target)

    def pair_done(k):
        if duo > 1:
            arrived(a4.at[k, 0 : duo - 1], f4.at[k])
        value = a4[k, 0].astype(F32)
        for j in range(1, duo):
            value = value + a4[k, j].astype(F32)
        piece = fin.at[pair_column(k, core)]
        piece[...] = value.astype(BF16)
        push(piece, piece, e5, f5, other)

    stages = (stage_core, stage_y, stage_x, stage_z, stage_cand)
    pair_stages = (pair_core, pair_x, pair_z, pair_y, pair_done)
    singles = a1.shape[0]
    step_time = 2.25
    plan = []
    for k in range(chunks):
        for stage, at in enumerate((0.0, 1.3 + 0.5 * k, 7.7 + 4.2 * k, 12.4 + 4.2 * k, 18.0 + 4.2 * k)):
            if stage:
                plan.append((at, stage, stages[stage], k))
    for k in range(singles):
        hp = chunks * duo + k - duos
        ready = step_time * (hp + 1) - 0.05 if hp >= 0 else 0.0
        for stage, at in enumerate((0.0, 1.2, 5.6, 11.0, 14.0)):
            if hp >= 0 or stage:
                plan.append((ready + at, 5 + stage, pair_stages[stage], k))
    plan.sort(key=lambda item: (item[0], item[1] % 5, item[3]))
    slots = [(step_time * hp + at, hp, place) for hp in range(duos)
             for place, at in enumerate((0.0, 1.3, step_time - 0.05))]
    homes = {}
    for item in plan:
        home = next(((hp, place) for at, hp, place in slots if at >= item[0] - 0.1), None)
        homes.setdefault(home, []).append(item)

    def keep(source, base):
        for t in range(duos):
            at = (base + t) // 2, (base + t) % 2
            grads[at] = source[:, t * lanes : (t + 1) * lanes].reshape(half, 2, rows, lanes)

    keep(lax.dot_general(ctx, out_grad, TN, preferred_element_type=F32).astype(BF16), duos)
    for k in range(duos - chunks * duo):
        pair_core(k)
    keep(lax.dot_general(u, spread, TN, preferred_element_type=F32).astype(BF16), 0)
    for k in range(chunks):
        stage_core(k)
    for i in range(pairs):
        for j in range(duos):
            dp_scr[j, i] = dp_scr[j, i] * sg[i : i + 1]

    def run(hp, place):
        with jax.named_scope('bw_run'):
            for step in range(duos):
                items = homes.get((step, place))
                if items:
                    @pl.when(hp == step)
                    def _():
                        for _, stage, act, k in items:
                            with jax.named_scope('in_%d_%d' % (stage, k)):
                                act(k)

    def differentiate(hp, i):
        probs = p_scr[hp, i].astype(F32)
        term = probs * dp_scr[hp, i][:, None, :]
        dlog = (term - probs * jnp.sum(term, axis=-1, keepdims=True)).astype(BF16)
        wide = jnp.concatenate([dlog[0], dlog[1]], axis=1)
        q2 = stack_halves(qk_scr[hp, i, :, :lanes], low, high)
        k2 = stack_halves(qk_scr[hp, i, :, lanes:], low, high)
        dq = jnp.dot(wide, k2, preferred_element_type=F32)
        dk = lax.dot_general(dlog.reshape(2 * seq, seq), q2, TN, preferred_element_type=F32)
        dqk_scr[i, :, :lanes] = dq.astype(BF16)
        dqk_scr[i, :, lanes:] = dk.astype(BF16)

    def backward_step(hp, carry):
        run(hp, 0)

        @pl.when(hp < duos)
        def _():
            with jax.named_scope('bw_block'):
                for i in range(pairs):
                    differentiate(hp, i)

        run(hp, 1)

        @pl.when(hp < duos)
        def _():
            with jax.named_scope('bw_dot'):
                grad = jnp.dot(nt_scr[...], dqk_scr[...].reshape(pairs * seq, 2 * lanes), preferred_element_type=F32)
                grads[duos + hp, 0] = grad[:, :lanes].reshape(half, 2, rows, lanes).astype(BF16)
                grads[duos + hp, 1] = grad[:, lanes:].reshape(half, 2, rows, lanes).astype(BF16)

        run(hp, 2)
        return carry

    lax.fori_loop(0, duos, backward_step, 0)
    def square(g):
        block = fin[g].astype(F32).reshape(rows // 8, 8, lanes)
        return jnp.sum(block * block, axis=0)

    part = jnp.zeros((8, lanes), F32)
    waiting = [k for k in range(chunks)]
    for _, stage, act, k in homes.get(None, []):
        if stage == 9 and waiting and k == singles - 1:
            part = finish_chunks(part, waiting, square)
            waiting = []
        with jax.named_scope('tail_%d_%d' % (stage, k)):
            act(k)
    if waiting:
        part = finish_chunks(part, waiting, square)
    part = jnp.where(core == 0, part, 0.0)
    for k in range(singles):
        part = part + square(pair_column(k, core))
    sq[...] = part
    mine = core * n + d
    r6[mine] = part
    targets = [(lax.rem(d + j, n), core) for j in range(1, n)] + [(lax.rem(d + j, n), 1 - core) for j in range(n)]
    for t, (to, to_core) in enumerate(targets):
        push(sq, r6.at[mine], t6, v6, (to, c - core + to_core))
    with jax.named_scope('fin_wait'):
        arrived(fin.at[0:singles], f5)
    store = pltpu.make_async_copy(fin, fin_hbm, b_sem)
    store.start()
    with jax.named_scope('drain'):
        kinds = early_rounds + late_rounds * duo
        arrived(w_scr.at[0:kinds, 0 : half - 1, 0], few_s)
        arrived(w_scr.at[0 : 3 * kinds // 2], many_s)
        arrived(ex_scr.at[0 : m - 1], ex_s)
        if chunks:
            arrived(r1, t1)
            arrived(r3, t3)
            arrived(fin.at[0 : chunks * (m - 1)], t5)
            if duo > 1:
                arrived(r2, t2)
            if half > 1:
                arrived(r4, t4)
        arrived(a1, e1)
        arrived(a2, e2)
        arrived(fin.at[0:singles], e5)
        if half > 1:
            arrived(a3, e3)
        if duo > 1:
            arrived(a4.at[:, 0 : duo - 1], e4)
    with jax.named_scope('sq_wait'):
        arrived(r6.at[0 : 2 * n - 1], v6)
        arrived(r6.at[0 : 2 * n - 1], t6)
    count = groups * lanes * n * rows
    squares = jnp.sum(r6[...], axis=0)
    squares = jnp.sum(jnp.sum(squares, axis=0, keepdims=True), axis=1, keepdims=True)
    loss_ref[0:1, :] = jnp.broadcast_to(1.0 / (jnp.sqrt(squares / count) + EPS), (1, lanes))
    store.wait()


def finish_kernel(fin, loss_in, out_ref, loss_ref):
    columns, _, lanes = fin.shape
    scale = loss_in[0:1, :]
    for at in range(columns):
        out_ref[:, at * lanes : (at + 1) * lanes] = fin[at].astype(F32) * scale
    for q in range(loss_ref.shape[0]):
        loss_ref[q] = jnp.max(loss_in[q + 1 : q + 2, :])


def shards(hidden, attn_weight, norm_gain, pos_bias, score_weight, pair_lengths, labels):
    queries, per, seq, width = hidden.shape
    pairs = queries * per
    heads = pos_bias.shape[0]
    n, m = lax.axis_size("dp"), lax.axis_size("cand")
    lanes = 2 * (width // heads)
    duos = heads // 2
    groups = 4 * duos
    rows, half, duo = width // n, n // 2, m // 2
    early = groups // 3
    early_rounds, late_rounds = early // 2, (groups - early) // m
    batch = 4 if pairs % 4 == 0 else 1
    hpad = -(-heads // 16) * 16
    chunks = max(duos // duo - 1, 1)
    singles = 2 * duos - chunks * duo
    near, far = max(duo - 1, 1), max(half - 1, 1)
    dma = pltpu.SemaphoreType.DMA
    vmem = pltpu.VMEM
    here = pl.BlockSpec(memory_space=pltpu.VMEM)
    away = pl.BlockSpec(memory_space=pl.ANY)
    small = pl.BlockSpec(memory_space=pltpu.SMEM)
    loss_rows = -(-(queries + 1) // 8) * 8
    fin, loss = pl.pallas_call(
        functools.partial(fused_kernel, n, m, early),
        in_specs=[away] * 7,
        out_specs=[away, here],
        out_shape=[
            jax.ShapeDtypeStruct((groups, rows, lanes), BF16),
            jax.ShapeDtypeStruct((loss_rows, lanes), F32),
        ],
        scratch_shapes=[
            pltpu.SMEM((queries, per), jnp.int32),
            pltpu.SMEM((queries, per), jnp.int32),
            vmem((width,), F32),
            vmem((width,), F32),
            dma((4,)),
            vmem((groups, rows, lanes), BF16),
            vmem((pairs, seq, width), BF16),
            vmem(pos_bias.shape, F32),
            vmem((groups, half, 2, rows, lanes), BF16),
            vmem((pairs, seq, width), BF16),
            vmem((width, pairs * seq), BF16),
            vmem((duos, pairs, seq, 2 * lanes), BF16),
            vmem((duos, pairs, 2, seq, seq), BF16),
            vmem((duos, pairs, 2, seq), F32),
            vmem((pairs, hpad, width), BF16),
            vmem((pairs, width), F32),
            vmem((m, 2 * pairs, lanes), F32),
            vmem((duos, pairs, 2, seq), F32),
            vmem((pairs, seq, 2 * lanes), BF16),
            vmem((2 * duos, 2, half, 2, rows, lanes), BF16),
            vmem((chunks, duo, half, 2, rows, lanes), BF16),
            vmem((chunks, duo, half, 2, rows, lanes), BF16),
            vmem((chunks, near, half, 2, rows, lanes), BF16),
            vmem((chunks, half, 2, rows, lanes), BF16),
            vmem((chunks, half, rows, lanes), BF16),
            vmem((chunks, half, rows, lanes), BF16),
            vmem((chunks, far, rows, lanes), BF16),
            vmem((singles, half, 2, rows, lanes), BF16),
            vmem((singles, half, 2, rows, lanes), BF16),
            vmem((singles, half, rows, lanes), BF16),
            vmem((singles, half, rows, lanes), BF16),
            vmem((singles, far, rows, lanes), BF16),
            vmem((singles, duo, rows, lanes), BF16),
            vmem((8, lanes), F32),
            vmem((2 * n, 8, lanes), F32),
            dma((pairs // batch,)), dma, dma((early_rounds,)), dma((late_rounds, duo)),
            dma((early_rounds, far)), dma((early_rounds,)), dma((late_rounds, far)), dma((late_rounds,)),
            dma((late_rounds, 2, near)), dma((early_rounds,)), dma((late_rounds,)), dma, dma, dma, dma,
            dma, dma((chunks,)), dma, dma((chunks,)), dma, dma((chunks,)), dma, dma((chunks,)), dma, dma, dma, dma,
            dma, dma((singles,)), dma, dma((singles,)), dma, dma((singles,)), dma, dma((singles,)), dma, dma,
        ],
        compiler_params=pltpu.CompilerParams(
            collective_id=0, has_side_effects=True, vmem_limit_bytes=VMEM_LIMIT
        ),
        name="fused_step",
    )(pair_lengths, labels, hidden.reshape(pairs, seq, width), attn_weight, norm_gain, pos_bias, score_weight)
    update, loss = pl.pallas_call(
        finish_kernel,
        grid=(FINISH,),
        in_specs=[
            pl.BlockSpec((groups // FINISH, rows, lanes), lambda i: (i, 0, 0)),
            pl.BlockSpec(loss.shape, lambda i: (0, 0)),
        ],
        out_specs=[pl.BlockSpec((rows, 4 * width // FINISH), lambda i: (0, i)), small],
        out_shape=[
            jax.ShapeDtypeStruct((rows, 4 * width), F32),
            jax.ShapeDtypeStruct((queries,), F32),
        ],
        name="finish",
    )(fin, loss)
    return (update, loss)


def solution(mesh):
    in_specs = (
        P("dp", "cand", None, None),
        P("dp", None),
        P(),
        P(),
        P(),
        P("dp", "cand"),
        P("dp", "cand"),
    )
    out_specs = (P("dp", None), P("dp"))
    return jax.shard_map(shards, mesh=mesh, in_specs=in_specs, out_specs=out_specs, check_vma=False)
```
